128 devices in a mesh: row: 16 (over y, z), col: 8 (over x, core).
Axes of the slice: x: 4, y: 4, z: 4, core: 2. Of those that a mesh axis runs over, the one named last changes fastest.
Arguments:
- root_rhs: bfloat16 [8, 8192], replicated, may hold values from -6 to 6
- diag_inv: bfloat16 [16, 512, 512], replicated, may hold values from -1 to 2
- tile_u: bfloat16 [16, 8, 1, 2, 128, 512], P('row', 'col'), may hold values from -0.1875 to 0.1875
- tile_v: bfloat16 [16, 8, 1, 2, 512, 128], P('row', 'col'), may hold values from -0.25 to 0.25
- tile_rank: int32 [16, 8, 1, 2], P('row', 'col'), may hold values from 16 to 128
- child_x: bfloat16 [128, 8, 512], P(('row', 'col')), may hold values from -6 to 6
- border_t: bfloat16 [128, 512, 1024], P(('row', 'col')), may hold values from -0.09375 to 0.09375
- child_inv: bfloat16 [128, 512, 512], P(('row', 'col')), may hold values from -1 to 2
- child_blocks: int32 [128, 8], P(('row', 'col')), may hold values from 0 to 63
Outputs:
- root_solution: float32 [8, 8192], P(None, ('row', 'col'))
- child_out: float32 [128, 8, 512], P(('row', 'col'))
The draws below stay inside these ranges and needn't reach their ends.
All inputs are finite; a program needn't handle non-finite values.
Results may differ from the reference program's by a relative error of at most 0.017.
Values sent between devices are 32-bit elements; how exact they have to be, the bound alone decides.
No kernel may reach another device: no remote copies, remote signals or barrier semaphores. Data moves between devices by JAX's collectives and lax.ppermute only.
A program may use at most 64 MiB of HBM per device.

```python
import math
import jax
import jax.numpy as jnp
import numpy as np
from jax import lax

NT = 16
TILE = 512
RHS = 8
RMAX = 128
BLK = 128
BB = 8
CSEP = 512
F = 8192
NB = 64
BORD = 1024
TR = 1
TC = 2
CHILDREN = 128
N_ROW = 16
N_COL = 8


def inverse_blocks(key, count, order):
    first, second_operand = jax.random.split(key, 2)
    diagonal = jax.random.uniform(first, (count, order), jnp.float32, 0.6, 1.2)
    spread = jnp.clip(jax.random.normal(second_operand, (count, order, order), jnp.float32), -6.0, 6.0)
    identity = jnp.eye(order, dtype=jnp.float32)
    blocks = spread * (0.5 / math.sqrt(order)) * (1.0 - identity) + identity[None] * diagonal[:, :, None]
    return blocks.astype(jnp.bfloat16)


def draw_diag_inv(key, part):
    return inverse_blocks(jax.random.fold_in(key, 11), NT, TILE)


def draw_child_inv(key, part):
    return inverse_blocks(jax.random.fold_in(key, 23), CHILDREN, CSEP)


def set_ends(entries, own_key, smallest, high):
    index_at = [jax.random.randint(jax.random.fold_in(own_key, axis), (), 0, length) for axis, length in enumerate(entries.shape)]
    longest = entries.shape.index(max(entries.shape))
    neighbour = index_at[:longest] + [(index_at[longest] + 1) % entries.shape[longest]] + index_at[longest + 1:]
    return entries.at[tuple(index_at)].set(smallest).at[tuple(neighbour)].set(high)


def block_scale(own_key, extent, cuts, least, high):
    def one(position, shards_of):
        steps = jax.random.uniform(jax.random.fold_in(jax.random.fold_in(own_key, 6), position), (shards_of,), jnp.float32, least / len(cuts), high / len(cuts))
        return jnp.repeat(jnp.exp(steps), extent[position] // shards_of).reshape((-1,) + (1,) * (len(extent) - position - 1))

    factor_of = one(*cuts[0])
    for cut in cuts[1:]:
        factor_of = factor_of * one(*cut)
    return factor_of


def rank_bounds(number_of, slope):
    weights = [(1 << 20) // math.isqrt(standing ** slope) + 1 for standing in range(1, number_of + 1)]
    scale = 1 + sum(weights) // (1 << 30)
    return np.cumsum(np.array([max(1, weight // scale) for weight in weights]))


def ranked(own_key, dims, amount, slope):
    table = rank_bounds(amount, slope)
    lot = jax.random.randint(jax.random.fold_in(own_key, 1), dims, 0, int(table[amount - 1]))
    standing = jnp.searchsorted(jnp.asarray(table, jnp.int32), lot, side="right")
    return jax.random.permutation(jax.random.fold_in(own_key, 2), amount)[standing].astype(jnp.int32)


def normal_values(stream_key, shape, scale, reach, cuts=(), kind=jnp.bfloat16):
    values = scale * jax.random.normal(stream_key, shape, jnp.float32)
    if cuts:
        values = values * block_scale(stream_key, shape, cuts, -0.22, 0.18)
    return jnp.clip(values, -reach, reach).astype(kind)


def setup_inputs(seed: int = 0) -> dict:
    splits = jax.random.split(jax.random.key(seed), 10)
    return {
        "root_rhs": normal_values(splits[0], (RHS, F), 1.0, 6.0),
        "diag_inv": draw_diag_inv(jax.random.fold_in(splits[9], 71), 0),
        "tile_u": normal_values(splits[2], (N_ROW, N_COL, TR, TC, RMAX, TILE), (RMAX * NT // 2) ** -0.5, 0.1875, ((0, 16), (1, 8))),
        "tile_v": normal_values(splits[3], (N_ROW, N_COL, TR, TC, TILE, RMAX), TILE ** -0.5, 0.25, ((0, 16), (1, 8))),
        "tile_rank": set_ends(jax.random.randint(splits[4], (N_ROW, N_COL, TR, TC), RMAX // 8, RMAX + 1), jax.random.fold_in(splits[4], 1), RMAX // 8, RMAX).astype(jnp.int32),
        "child_x": normal_values(splits[5], (CHILDREN, RHS, CSEP), 1.0, 6.0, ((0, 128),)),
        "border_t": normal_values(splits[6], (CHILDREN, CSEP, BORD), (CSEP * BB) ** -0.5, 0.09375, ((0, 128),)),
        "child_inv": draw_child_inv(jax.random.fold_in(splits[9], 71), 0),
        "child_blocks": set_ends(ranked(splits[8], (CHILDREN, BB), NB, 1), jax.random.fold_in(splits[8], 3), 0, NB - 1).astype(jnp.int32),
    }


def rounded_value(values):
    return lax.optimization_barrier(values.astype(jnp.bfloat16)).astype(jnp.float32)


def reference(root_rhs, diag_inv, tile_u, tile_v, tile_rank, child_x, border_t, child_inv, child_blocks):
    highest_precision = lax.Precision.HIGHEST
    upward = jnp.einsum('crs,csb->crb', child_x.astype(jnp.float32), border_t.astype(jnp.float32))
    pieces = upward.reshape(CHILDREN, RHS, BB, BLK).transpose(1, 0, 2, 3).reshape(RHS, CHILDREN * BB, BLK)
    flat_blocks = child_blocks.reshape(-1).astype(jnp.int32)
    dense_sum = jnp.zeros((RHS, NB, BLK), jnp.float32).at[:, flat_blocks, :].add(pieces)
    child_sum = dense_sum.reshape(RHS, NT, TILE)
    right_side = root_rhs.astype(jnp.float32).reshape(RHS, NT, TILE)
    inverses = diag_inv.astype(jnp.float32)
    rank_iota = jnp.arange(RMAX)
    tile_ids = jnp.arange(NT)
    solved_rows = jnp.zeros((RHS, NT, TILE), jnp.float32)
    for column in range(NT):
        owner_row, owner_slot = column % N_ROW, column // N_ROW
        left_rows = tile_u[owner_row, :, owner_slot].transpose(1, 0, 2, 3).reshape(NT, RMAX, TILE)
        right_row_indices = tile_v[owner_row, :, owner_slot].transpose(1, 0, 2, 3).reshape(NT, TILE, RMAX)
        rank_rows = tile_rank[owner_row, :, owner_slot].T.reshape(NT)
        live_mask = (rank_iota[None, :] < rank_rows[:, None]) & (tile_ids[:, None] < column)
        coefficient_values = jnp.einsum('gic,icw->giw', rounded_value(solved_rows), right_row_indices.astype(jnp.float32))
        coefficient_values = rounded_value(jnp.where(live_mask[None], coefficient_values, 0.0))
        partial_value = jnp.einsum('rkq,kqt->rt', coefficient_values, left_rows.astype(jnp.float32))
        row_total = partial_value + child_sum[:, column]
        fresh = jnp.dot(right_side[:, column] - row_total, inverses[column], precision=highest_precision)
        solved_rows = solved_rows.at[:, column].set(fresh)
    result = jnp.zeros((RHS, NT, TILE), jnp.float32)
    for column in reversed(range(NT)):
        owner_col, owner_slot = column % N_COL, column // N_COL
        left_cols = tile_u[:, owner_col, :, owner_slot].transpose(1, 0, 2, 3).reshape(NT, RMAX, TILE)
        right_cols = tile_v[:, owner_col, :, owner_slot].transpose(1, 0, 2, 3).reshape(NT, TILE, RMAX)
        rank_cols = tile_rank[:, owner_col, :, owner_slot].T.reshape(NT)
        live_mask = (rank_iota[None, :] < rank_cols[:, None]) & (tile_ids[:, None] > column)
        coefficient_values = jnp.einsum('rit,iqt->riq', rounded_value(result), left_cols.astype(jnp.float32))
        coefficient_values = rounded_value(jnp.where(live_mask[None], coefficient_values, 0.0))
        partial_value = jnp.einsum('riq,itq->rt', coefficient_values, right_cols.astype(jnp.float32))
        fresh = jnp.dot(solved_rows[:, column] - partial_value, inverses[column].T, precision=highest_precision)
        result = result.at[:, column].set(fresh)
    root_solution = result.reshape(RHS, F)
    gathered = result.reshape(RHS, NB, BLK)[:, flat_blocks, :].reshape(RHS, CHILDREN, BB * BLK)
    returned = jnp.einsum('rcb,csb->crs', rounded_value(gathered), border_t.astype(jnp.float32))
    child_out = child_x.astype(jnp.float32) - jnp.einsum('crs,cst->crt', returned, child_inv.astype(jnp.float32), precision=highest_precision)
    return root_solution, child_out
```

```python
import functools

import jax
import jax.numpy as jnp
from jax import lax
from jax.experimental import pallas as pl
from jax.experimental.layout import Layout, with_layout_constraint
from jax.experimental.pallas import tpu as pltpu
from jax.sharding import Mesh
from jax.sharding import PartitionSpec as P

BLK = 128
BB = 8
ROW = ("y", "z")
COL = ("x", "c")
ALL = ("y", "z", "x", "c")
HALF = 8
BF = jnp.bfloat16
F32 = jnp.float32
ROWS = Layout((0, 1))


def copies(v, axis):
    n = lax.axis_size(axis)
    stacked = jnp.broadcast_to(v, (n, *v.shape))
    return lax.all_to_all(stacked, axis, split_axis=0, concat_axis=0, tiled=True)


def dot_nn(a, b):
    return lax.dot_general(a, b, (((1,), (0,)), ((), ())), preferred_element_type=F32)


def dot_nt(a, b):
    return lax.dot_general(a, b, (((1,), (1,)), ((), ())), preferred_element_type=F32)


def exact(dot, a, b):
    high = a.astype(BF)
    low = (a - high.astype(F32)).astype(BF)
    both = dot(jnp.concatenate([high, low], axis=0), b)
    n = a.shape[0]
    return both[:n] + both[n:]


def first_tile(row):
    return row * (row - 1) // 2


class Leaf:
    def __init__(self, half, tiles, inv, left, right, diag, sems, dsems, order):
        self.left, self.right, self.diag = left, right, diag
        self.copies = {}
        for n in order:
            items = [pltpu.make_async_copy(inv.at[HALF * half + n], diag.at[n], dsems.at[n])]
            if n:
                base = first_tile(n)
                at = 64 * half + 8 * n
                mirrored = 64 * half + 8 * (7 - n) + 8 - n
                items.append(
                    pltpu.make_async_copy(
                        tiles.at[pl.ds(at, n)], left.at[pl.ds(base, n)], sems.at[0, n]
                    )
                )
                items.append(
                    pltpu.make_async_copy(
                        tiles.at[pl.ds(mirrored, n)], right.at[pl.ds(base, n)], sems.at[1, n]
                    )
                )
            self.copies[n] = items
        for n in order:
            for item in self.copies[n]:
                item.start()

    def wait(self, n):
        for item in self.copies[n]:
            item.wait()

    def u(self, i, k):
        return self.left[first_tile(i) + k].astype(BF)

    def vt(self, i, k):
        return self.right[first_tile(i) + i - 1 - k].astype(BF)


def forward(leaf, rhs_ref, wait=True):
    solved = []
    narrow = []
    for i in range(HALF):
        if wait:
            leaf.wait(i)
        acc = rhs_ref[i]
        for k in range(i):
            p = dot_nt(narrow[k], leaf.vt(i, k)).astype(BF)
            acc = acc - dot_nn(p, leaf.u(i, k))
        x = exact(dot_nn, acc, leaf.diag[i])
        solved.append(x)
        narrow.append(x.astype(BF))
    return solved


def backward(leaf, rhs, wait):
    solved = {}
    narrow = {}
    for j in reversed(range(HALF)):
        if wait:
            leaf.wait(j)
        acc = rhs[j]
        for i in reversed(range(j + 1, HALF)):
            q = dot_nt(narrow[i], leaf.u(i, j)).astype(BF)
            acc = acc - dot_nn(q, leaf.vt(i, j))
        z = exact(dot_nt, acc, leaf.diag[j])
        solved[j] = z
        narrow[j] = z.astype(BF)
    return solved


def forward_kernel(half, tiles, inv, rhs, out, left, right, diag, sems, dsems):
    leaf = Leaf(half, tiles, inv, left, right, diag, sems, dsems, range(HALF))
    for i, x in enumerate(forward(leaf, rhs)):
        out[i] = x


def both_kernel(half, tiles, inv, rhs, out, left, right, diag, sems, dsems):
    leaf = Leaf(half, tiles, inv, left, right, diag, sems, dsems, range(HALF))
    solved = forward(leaf, rhs)
    for j, z in backward(leaf, solved, False).items():
        out[j] = z


def backward_kernel(half, tiles, inv, rhs, out, left, right, diag, sems, dsems):
    leaf = Leaf(half, tiles, inv, left, right, diag, sems, dsems, range(HALF)[::-1])
    for j, z in backward(leaf, [rhs[j] for j in range(HALF)], True).items():
        out[j] = z


def in_hbm(v):
    return pltpu.with_memory_space_constraint(v, pltpu.HBM)


def leaf_call(body, half, tiles, inv, rhs):
    count = first_tile(HALF)
    shape = tiles.shape[1:]
    tile = inv.shape[1]
    return pl.pallas_call(
        functools.partial(body, half),
        out_shape=jax.ShapeDtypeStruct(rhs.shape, F32),
        in_specs=[
            pl.BlockSpec(memory_space=pltpu.HBM),
            pl.BlockSpec(memory_space=pltpu.HBM),
            pl.BlockSpec(memory_space=pltpu.VMEM),
        ],
        out_specs=pl.BlockSpec(memory_space=pltpu.VMEM),
        scratch_shapes=[
            pltpu.VMEM((count, *shape), F32),
            pltpu.VMEM((count, *shape), F32),
            pltpu.VMEM((HALF, tile, tile), BF),
            pltpu.SemaphoreType.DMA((2, HALF)),
            pltpu.SemaphoreType.DMA((HALF,)),
        ],
        compiler_params=pltpu.CompilerParams(vmem_limit_bytes=40 * 1024 * 1024),
    )(in_hbm(tiles), in_hbm(inv), rhs)


def per_device(
    root_rhs, diag_inv, tile_u, tile_v, tile_rank, child_x, border_t, child_inv, child_blocks
):
    my_row = lax.axis_index(ROW)
    my_col = lax.axis_index(COL)
    ntile = diag_inv.shape[0]
    tile = diag_inv.shape[1]
    rhs_count = root_rhs.shape[0]
    rank_max = tile_u.shape[4]
    n_child = child_x.shape[0]
    nblk = ntile * tile // BLK
    ndev = lax.axis_size(ALL)
    upper = my_row >= HALF
    in_half = my_row % HALF

    left = tile_u[0, 0, 0]
    live = jnp.arange(rank_max)[None, None, :] < tile_rank[0, 0, 0][:, None, None]
    right = jnp.where(live, tile_v[0, 0, 0].astype(F32), 0.0)

    has_leaf = my_col < in_half
    leaf_u = jnp.where(upper, left[1], left[0]).astype(F32)
    leaf_vt = jnp.where(upper, right[1], right[0]).T
    pairs = []
    for r in range(16):
        for c in range(8):
            partner = (r // 8 * 8 + 7 - r % 8) * 8 + 7 - c
            pairs.append((r * 8 + c, partner))
    from_partner = lax.ppermute(with_layout_constraint(leaf_vt, ROWS), ALL, pairs)
    share = with_layout_constraint(jnp.where(has_leaf, leaf_u, from_partner), ROWS)
    tiles = lax.all_gather(share, ALL)

    upward = jnp.einsum("crs,csb->crb", child_x, border_t, preferred_element_type=F32)
    pieces = (
        upward.reshape(n_child, rhs_count, BB, BLK)
        .transpose(1, 0, 2, 3)
        .reshape(rhs_count, n_child * BB, BLK)
    )
    flat_blocks = child_blocks.reshape(-1)
    dense = jnp.zeros((rhs_count, nblk, BLK), F32).at[:, flat_blocks, :].add(pieces)
    width = ntile * tile // ndev
    parts = dense.reshape(rhs_count, ndev, width).transpose(1, 0, 2)
    mine = lax.all_to_all(parts, ALL, split_axis=0, concat_axis=0, tiled=True).sum(axis=0)
    child_sum = copies(mine, ALL).reshape(ndev, rhs_count, width)
    child_sum = child_sum.transpose(1, 0, 2).reshape(rhs_count, ntile, tile).transpose(1, 0, 2)
    rhs = root_rhs.reshape(rhs_count, ntile, tile).transpose(1, 0, 2).astype(F32) - child_sum

    x_low = leaf_call(forward_kernel, 0, tiles, diag_inv, rhs[:HALF])
    v0 = right[0].astype(BF)
    u0 = left[0]
    x_own = lax.dynamic_index_in_dim(x_low, my_col, 0, keepdims=False).astype(BF)
    p = dot_nn(x_own, v0).astype(BF)
    given = jnp.where(upper, dot_nn(p, u0), 0.0)
    row_sum = copies(given, COL).reshape(8, rhs_count, tile).sum(axis=0)
    row_sums = copies(row_sum, ROW).reshape(16, rhs_count, tile)
    z_high = leaf_call(both_kernel, 1, tiles, diag_inv, rhs[HALF:] - row_sums[HALF:])

    z_own = lax.dynamic_index_in_dim(z_high, in_half, 0, keepdims=False).astype(BF)
    q = dot_nt(z_own, u0).astype(BF)
    given = jnp.where(upper, dot_nt(q, v0), 0.0)
    col_sum = copies(given, ROW).reshape(16, rhs_count, tile)[HALF:].sum(axis=0)
    col_sums = copies(col_sum, COL).reshape(8, rhs_count, tile)
    z_low = leaf_call(backward_kernel, 0, tiles, diag_inv, x_low - col_sums)
    result = jnp.concatenate([z_low, z_high], axis=0).transpose(1, 0, 2)
    result = result.reshape(rhs_count, ntile * tile)

    start = (my_row * 8 + my_col) * width
    root_part = lax.dynamic_slice_in_dim(result, start, width, 1)
    gathered = result.reshape(rhs_count, nblk, BLK)[:, flat_blocks, :]
    gathered = gathered.reshape(rhs_count, n_child, BB * BLK).astype(BF)
    returned = jnp.einsum("rcb,csb->crs", gathered, border_t, preferred_element_type=F32)
    child_out = child_x.astype(F32) - jnp.einsum(
        "crs,cst->crt", returned, child_inv.astype(F32)
    )
    return (root_part, child_out)


def solution(mesh):
    finer = Mesh(mesh.devices.reshape(4, 4, 4, 2), ALL)
    in_specs = (
        P(),
        P(),
        P(ROW, COL, None, None, None, None),
        P(ROW, COL, None, None, None, None),
        P(ROW, COL, None, None),
        P(ALL, None, None),
        P(ALL, None, None),
        P(ALL, None, None),
        P(ALL, None),
    )
    out_specs = (P(None, ALL), P(ALL, None, None))
    return jax.shard_map(
        per_device, mesh=finer, in_specs=in_specs, out_specs=out_specs, check_vma=False
    )
```

```python
import functools

import jax
import jax.numpy as jnp
from jax import lax
from jax.experimental import pallas as pl
from jax.experimental.layout import Layout, with_layout_constraint
from jax.experimental.pallas import tpu as pltpu
from jax.sharding import Mesh
from jax.sharding import PartitionSpec as P

BLK = 128
BB = 8
ROW = ("y", "z")
COL = ("x", "c")
ALL = ("y", "z", "x", "c")
HALF = 8
BF = jnp.bfloat16
F32 = jnp.float32
ROWS = Layout((0, 1))


def copies(v, axis):
    n = lax.axis_size(axis)
    stacked = jnp.broadcast_to(v, (n, *v.shape))
    return lax.all_to_all(stacked, axis, split_axis=0, concat_axis=0, tiled=True)


def dot_nn(a, b):
    return lax.dot_general(a, b, (((1,), (0,)), ((), ())), preferred_element_type=F32)


def dot_nt(a, b):
    return lax.dot_general(a, b, (((1,), (1,)), ((), ())), preferred_element_type=F32)


def exact(dot, a, b):
    high = a.astype(BF)
    low = (a - high.astype(F32)).astype(BF)
    both = dot(jnp.concatenate([high, low], axis=0), b)
    n = a.shape[0]
    return both[:n] + both[n:]


def first_tile(row):
    return row * (row - 1) // 2


SLOTS = 3


class Leaf:
    def __init__(self, rows, where, first, tiles, inv, stage, left, right, diag, sems, dsems):
        self.rows, self.stage, self.left, self.right, self.diag = rows, stage, left, right, diag
        self.inverse = [
            pltpu.make_async_copy(inv.at[first + n], diag.at[n], dsems.at[n]) for n in range(rows)
        ]
        self.moves = {}
        for i in range(rows):
            self.moves[i] = []
            for k in range(i):
                for side in range(2):
                    array, index = where(i, k)[side]
                    self.moves[i].append(
                        pltpu.make_async_copy(
                            tiles[array].at[index],
                            stage.at[i % SLOTS, k, side],
                            sems.at[side, first_tile(i) + k],
                        )
                    )

    def start(self, i):
        if 0 <= i < self.rows:
            self.inverse[i].start()
            for move in self.moves[i]:
                move.start()

    def column(self, j):
        return sum(self.rows - 1 - m for m in range(j))

    def load(self, i, step=1):
        self.inverse[i].wait()
        for move in self.moves[i]:
            move.wait()
        for k in range(i):
            self.left[first_tile(i) + k] = self.stage[i % SLOTS, k, 0].astype(BF)
            self.right[self.column(k) + i - k - 1] = self.stage[i % SLOTS, k, 1].astype(BF)
        self.start(i + step * SLOTS)

    def u(self, i, k, count=1):
        at = first_tile(i) + k
        return self.left[at : at + count].reshape(-1, self.left.shape[2])

    def vt(self, i, k, count=1):
        at = self.column(k) + i - k - 1
        return self.right[at : at + count].reshape(-1, self.right.shape[2])


def forward(leaf, rhs):
    solved, narrow = [], []
    for i in range(min(SLOTS, leaf.rows)):
        leaf.start(i)
    leaf.load(0)
    partial = rhs[0]
    last = None
    for i in range(leaf.rows):
        acc = partial
        if i:
            acc = acc - dot_nn(last, leaf.u(i, i - 1))
        x = exact(dot_nn, acc, leaf.diag[i])
        if i + 1 < leaf.rows:
            leaf.load(i + 1)
            partial = rhs[i + 1]
            if i:
                known = [dot_nt(narrow[k], leaf.vt(i + 1, k)).astype(BF) for k in range(i)]
                partial = partial - dot_nn(jnp.concatenate(known, axis=1), leaf.u(i + 1, 0, i))
        solved.append(x)
        narrow.append(x.astype(BF))
        if i + 1 < leaf.rows:
            last = dot_nt(narrow[i], leaf.vt(i + 1, i)).astype(BF)
    return solved


def backward(leaf, rhs, load):
    rows = leaf.rows
    if load:
        for i in range(min(SLOTS, rows)):
            leaf.start(rows - 1 - i)
        leaf.load(rows - 1, -1)
    width = leaf.left.shape[1]
    solved = {}
    waiting = {j: [] for j in range(rows)}
    partial = rhs[rows - 1]
    last = None
    for j in reversed(range(rows)):
        acc = partial
        if j + 1 < rows:
            acc = acc - dot_nn(last, leaf.vt(j + 1, j))
        z = exact(dot_nt, acc, leaf.diag[j])
        if j:
            if load:
                leaf.load(j - 1, -1)
            partial = rhs[j - 1]
            if waiting[j - 1]:
                known = jnp.concatenate(waiting[j - 1][::-1], axis=1)
                partial = partial - dot_nn(known, leaf.vt(j + 1, j - 1, rows - 1 - j))
        solved[j] = z
        narrow = z.astype(BF)
        if j:
            last = dot_nt(narrow, leaf.u(j, j - 1)).astype(BF)
        if j > 1:
            others = dot_nt(narrow, leaf.u(j, 0, j - 1)).astype(BF)
            for k in range(j - 1):
                waiting[k].append(others[:, k * width : (k + 1) * width])
    return solved


def solve_kernel(rows, where, first, sweeps, narrays, *refs):
    tiles = refs[:narrays]
    inv, rhs, out, stage, left, right, diag, sems, dsems = refs[narrays:]
    leaf = Leaf(rows, where, first, tiles, inv, stage, left, right, diag, sems, dsems)
    values = [rhs[i] for i in range(rows)]
    if sweeps != "backward":
        values = forward(leaf, values)
    if sweeps != "forward":
        values = backward(leaf, values, sweeps == "backward")
    for i in range(rows):
        out[i] = values[i]


def in_hbm(v):
    return pltpu.with_memory_space_constraint(v, pltpu.HBM)


def solve(sweeps, rows, where, first, arrays, inv, rhs):
    count = first_tile(rows)
    shape = arrays[0].shape[1:]
    tile = inv.shape[1]
    return pl.pallas_call(
        functools.partial(solve_kernel, rows, where, first, sweeps, len(arrays)),
        out_shape=jax.ShapeDtypeStruct(rhs.shape, F32),
        in_specs=[pl.BlockSpec(memory_space=pltpu.HBM)] * (len(arrays) + 1)
        + [pl.BlockSpec(memory_space=pltpu.VMEM)],
        out_specs=pl.BlockSpec(memory_space=pltpu.VMEM),
        scratch_shapes=[
            pltpu.VMEM((SLOTS, rows - 1, 2, *shape), F32),
            pltpu.VMEM((count, *shape), BF),
            pltpu.VMEM((count, *shape), BF),
            pltpu.VMEM((rows, tile, tile), BF),
            pltpu.SemaphoreType.DMA((2, count)),
            pltpu.SemaphoreType.DMA((rows,)),
        ],
        compiler_params=pltpu.CompilerParams(vmem_limit_bytes=50 * 1024 * 1024),
    )(*[in_hbm(v) for v in arrays], in_hbm(inv), rhs)


def in_gathered(half, i, k):
    at = 64 * half
    return (0, at + 8 * i + k), (0, at + 8 * (7 - i) + 7 - k)


def per_device(
    root_rhs, diag_inv, tile_u, tile_v, tile_rank, child_x, border_t, child_inv, child_blocks
):
    my_row = lax.axis_index(ROW)
    my_col = lax.axis_index(COL)
    ntile = diag_inv.shape[0]
    tile = diag_inv.shape[1]
    rhs_count = root_rhs.shape[0]
    rank_max = tile_u.shape[4]
    n_child = child_x.shape[0]
    nblk = ntile * tile // BLK
    ndev = lax.axis_size(ALL)
    upper = my_row >= HALF
    in_half = my_row % HALF

    left = tile_u[0, 0, 0]
    live = jnp.arange(rank_max)[None, None, :] < tile_rank[0, 0, 0][:, None, None]
    right = jnp.where(live, tile_v[0, 0, 0].astype(F32), 0.0)

    has_leaf = my_col < in_half
    leaf_u = jnp.where(upper, left[1], left[0]).astype(F32)
    leaf_vt = jnp.where(upper, right[1], right[0]).T
    pairs = []
    for r in range(16):
        for c in range(8):
            partner = (r // 8 * 8 + 7 - r % 8) * 8 + 7 - c
            pairs.append((r * 8 + c, partner))
    from_partner = lax.ppermute(with_layout_constraint(leaf_vt, ROWS), ALL, pairs)
    share = with_layout_constraint(jnp.where(has_leaf, leaf_u, from_partner), ROWS)
    tiles = lax.all_gather(share, ALL)

    upward = jnp.einsum("crs,csb->crb", child_x, border_t, preferred_element_type=F32)
    pieces = (
        upward.reshape(n_child, rhs_count, BB, BLK)
        .transpose(1, 0, 2, 3)
        .reshape(rhs_count, n_child * BB, BLK)
    )
    flat_blocks = child_blocks.reshape(-1)
    dense = jnp.zeros((rhs_count, nblk, BLK), F32).at[:, flat_blocks, :].add(pieces)
    width = ntile * tile // ndev
    parts = dense.reshape(rhs_count, ndev, width).transpose(1, 0, 2)
    mine = lax.all_to_all(parts, ALL, split_axis=0, concat_axis=0, tiled=True).sum(axis=0)
    child_sum = copies(mine, ALL).reshape(ndev, rhs_count, width)
    child_sum = child_sum.transpose(1, 0, 2).reshape(rhs_count, ntile, tile).transpose(1, 0, 2)
    rhs = root_rhs.reshape(rhs_count, ntile, tile).transpose(1, 0, 2).astype(F32) - child_sum

    low = functools.partial(in_gathered, 0)
    high = functools.partial(in_gathered, 1)
    x_low = solve("forward", HALF, low, 0, [tiles], diag_inv, rhs[:HALF])
    v0 = right[0].astype(BF)
    u0 = left[0]
    x_own = lax.dynamic_index_in_dim(x_low, my_col, 0, keepdims=False).astype(BF)
    p = dot_nn(x_own, v0).astype(BF)
    given = jnp.where(upper, dot_nn(p, u0), 0.0)
    row_sum = copies(given, COL).reshape(8, rhs_count, tile).sum(axis=0)
    row_sums = copies(row_sum, ROW).reshape(16, rhs_count, tile)
    given_high = rhs[HALF:] - row_sums[HALF:]
    z_high = solve("both", HALF, high, HALF, [tiles], diag_inv, given_high)

    z_own = lax.dynamic_index_in_dim(z_high, in_half, 0, keepdims=False).astype(BF)
    q = dot_nt(z_own, u0).astype(BF)
    given = jnp.where(upper, dot_nt(q, v0), 0.0)
    col_sum = copies(given, ROW).reshape(16, rhs_count, tile)[HALF:].sum(axis=0)
    col_sums = copies(col_sum, COL).reshape(8, rhs_count, tile)
    z_low = solve("backward", HALF, low, 0, [tiles], diag_inv, x_low - col_sums)
    result = jnp.concatenate([z_low, z_high], axis=0).transpose(1, 0, 2)
    result = result.reshape(rhs_count, ntile * tile)

    start = (my_row * 8 + my_col) * width
    root_part = lax.dynamic_slice_in_dim(result, start, width, 1)
    gathered = result.reshape(rhs_count, nblk, BLK)[:, flat_blocks, :]
    gathered = gathered.reshape(rhs_count, n_child, BB * BLK).astype(BF)
    returned = jnp.einsum("rcb,csb->crs", gathered, border_t, preferred_element_type=F32)
    child_out = child_x.astype(F32) - jnp.einsum(
        "crs,cst->crt", returned, child_inv.astype(F32)
    )
    return (root_part, child_out)


def solution(mesh):
    finer = Mesh(mesh.devices.reshape(4, 4, 4, 2), ALL)
    in_specs = (
        P(),
        P(),
        P(ROW, COL, None, None, None, None),
        P(ROW, COL, None, None, None, None),
        P(ROW, COL, None, None),
        P(ALL, None, None),
        P(ALL, None, None),
        P(ALL, None, None),
        P(ALL, None),
    )
    out_specs = (P(None, ALL), P(ALL, None, None))
    return jax.shard_map(
        per_device, mesh=finer, in_specs=in_specs, out_specs=out_specs, check_vma=False
    )
```

```python
import functools

import jax
import jax.numpy as jnp
from jax import lax
from jax.experimental import pallas as pl
from jax.experimental.layout import Layout, with_layout_constraint
from jax.experimental.pallas import tpu as pltpu
from jax.sharding import Mesh
from jax.sharding import PartitionSpec as P

BLK = 128
BB = 8
ROW = ("yh", "yl", "z")
HALF_ROW = ("yl", "z")
COL = ("x", "c")
PLANE = ("z", "x", "c")
ALL = ("yh", "yl", "z", "x", "c")
HALF = 8
BF = jnp.bfloat16
F32 = jnp.float32
ROWS = Layout((0, 1))


def copies(v, axis):
    n = lax.axis_size(axis)
    stacked = jnp.broadcast_to(v, (n, *v.shape))
    return lax.all_to_all(stacked, axis, split_axis=0, concat_axis=0, tiled=True)


def dot_nn(a, b):
    return lax.dot_general(a, b, (((1,), (0,)), ((), ())), preferred_element_type=F32)


def dot_nt(a, b):
    return lax.dot_general(a, b, (((1,), (1,)), ((), ())), preferred_element_type=F32)


def exact(dot, a, b):
    high = a.astype(BF)
    low = (a - high.astype(F32)).astype(BF)
    both = dot(jnp.concatenate([high, low], axis=0), b)
    n = a.shape[0]
    return both[:n] + both[n:]


def first_tile(row):
    return row * (row - 1) // 2


SLOTS = 3
TILES = first_tile(HALF)
SPARE = {(1, 0): (1, 7), (2, 0): (2, 6), (2, 1): (2, 7), (3, 0): (0, 6), (3, 1): (3, 7), (3, 2): (0, 7)}


def spot(plane, i, k):
    z = i % 4
    own = i // 4 == plane
    if own or (plane == 0 and k >= z):
        return 8 * z + k
    z, k = SPARE[z, k]
    return 8 * z + k


def plane_pairs():
    pairs = []
    for half in range(2):
        for i in range(HALF):
            for k in range(i):
                plane = i // 4
                source = 64 * half + 32 * plane + spot(plane, i, k)
                target = 64 * half + 32 * (1 - plane) + spot(1 - plane, i, k)
                pairs.append((source, target))
    return pairs


class Leaf:
    def __init__(self, left, right, diag):
        self.left, self.right, self.diag = left, right, diag

    def column(self, j):
        return sum(HALF - 1 - m for m in range(j))

    def u(self, i, k, count=1):
        at = first_tile(i) + k
        return self.left[at : at + count].reshape(-1, self.left.shape[2])

    def vt(self, i, k, count=1):
        at = self.column(k) + i - k - 1
        return self.right[at : at + count].reshape(-1, self.right.shape[2])


class Moves:
    def __init__(self, rows):
        self.rows = rows

    def start(self, i):
        for move in self.rows.get(i, []):
            move.start()

    def wait(self, i):
        for move in self.rows.get(i, []):
            move.wait()


def inverse_moves(leaf, first, inv, sems):
    return Moves(
        {
            n: [pltpu.make_async_copy(inv.at[first + n], leaf.diag.at[n], sems.at[n])]
            for n in range(HALF)
        }
    )


def factor_moves(leaf, kept_left, kept_right, lsems, rsems, keep):
    rows = {}
    for i in range(1, HALF):
        at = first_tile(i)
        pairs = [(kept_left.at[pl.ds(at, i)], leaf.left.at[pl.ds(at, i)], lsems.at[i])]
        for k in range(i):
            place = leaf.column(k) + i - k - 1
            pairs.append((kept_right.at[place], leaf.right.at[place], rsems.at[place]))
        rows[i] = [
            pltpu.make_async_copy(*((b, a) if keep else (a, b)), sem) for a, b, sem in pairs
        ]
    return Moves(rows)


class Loader:
    def __init__(self, leaf, place, tiles, inv, kept, stage, sems, dsems, lsems, rsems):
        self.leaf, self.stage = leaf, stage
        rows = {}
        for i in range(1, HALF):
            rows[i] = []
            for k in range(i):
                one, two = spot(0, i, k), spot(1, i, k)
                rows[i].append(
                    pltpu.make_async_copy(
                        tiles.at[one + place[0] * (two - one)],
                        stage.at[i % SLOTS, k],
                        sems.at[first_tile(i) + k],
                    )
                )
        self.tiles = Moves(rows)
        self.inverse = inverse_moves(leaf, HALF * place[1], inv, dsems)
        self.kept = factor_moves(leaf, *kept, lsems, rsems, True)
        for i in range(SLOTS):
            self.start(i)
        self(0)

    def start(self, i):
        self.inverse.start(i)
        self.tiles.start(i)

    def __call__(self, i):
        leaf = self.leaf
        rank = leaf.left.shape[1]
        self.inverse.wait(i)
        self.tiles.wait(i)
        for k in range(i):
            leaf.left[first_tile(i) + k] = self.stage[i % SLOTS, k, :rank].astype(BF)
            leaf.right[leaf.column(k) + i - k - 1] = self.stage[i % SLOTS, k, rank:].astype(BF)
        self.kept.start(i)
        if i + SLOTS < HALF:
            self.start(i + SLOTS)

    def finish(self):
        for i in range(HALF):
            self.kept.wait(i)


class Reloader:
    def __init__(self, leaf, place, inv, kept, dsems, lsems, rsems, order):
        self.inverse = inverse_moves(leaf, HALF * place[1], inv, dsems)
        self.factors = factor_moves(leaf, *kept, lsems, rsems, False)
        for i in order:
            self.inverse.start(i)
            self.factors.start(i)
        self(order[0])

    def __call__(self, i):
        self.inverse.wait(i)
        self.factors.wait(i)


def forward(leaf, rhs, load=None):
    solved, narrow = [], []
    partial = rhs[0]
    last = None
    for i in range(HALF):
        acc = partial
        if i:
            acc = acc - dot_nn(last, leaf.u(i, i - 1))
        x = exact(dot_nn, acc, leaf.diag[i])
        if i + 1 < HALF:
            if load:
                load(i + 1)
            partial = rhs[i + 1]
            if i:
                known = [dot_nt(narrow[k], leaf.vt(i + 1, k)).astype(BF) for k in range(i)]
                partial = partial - dot_nn(jnp.concatenate(known, axis=1), leaf.u(i + 1, 0, i))
        solved.append(x)
        narrow.append(x.astype(BF))
        if i + 1 < HALF:
            last = dot_nt(narrow[i], leaf.vt(i + 1, i)).astype(BF)
    return solved


def backward(leaf, rhs, load=None):
    width = leaf.left.shape[1]
    solved = [None] * HALF
    waiting = {j: [] for j in range(HALF)}
    partial = rhs[HALF - 1]
    last = None
    for j in reversed(range(HALF)):
        acc = partial
        if j + 1 < HALF:
            acc = acc - dot_nn(last, leaf.vt(j + 1, j))
        z = exact(dot_nt, acc, leaf.diag[j])
        if j:
            if load:
                load(j - 1)
            partial = rhs[j - 1]
            if waiting[j - 1]:
                known = jnp.concatenate(waiting[j - 1][::-1], axis=1)
                partial = partial - dot_nn(known, leaf.vt(j + 1, j - 1, HALF - 1 - j))
        solved[j] = z
        narrow = z.astype(BF)
        if j:
            last = dot_nt(narrow, leaf.u(j, j - 1)).astype(BF)
        if j > 1:
            others = dot_nt(narrow, leaf.u(j, 0, j - 1)).astype(BF)
            for k in range(j - 1):
                waiting[k].append(others[:, k * width : (k + 1) * width])
    return solved


def put(out, values):
    for i in range(HALF):
        out[i] = values[i]


def load_kernel(place, tiles, inv, rhs, out, kept_left, kept_right, stage, *scratch):
    left, right, diag, sems, dsems, lsems, rsems = scratch
    leaf = Leaf(left, right, diag)
    kept = (kept_left, kept_right)
    load = Loader(leaf, place, tiles, inv, kept, stage, sems, dsems, lsems, rsems)
    put(out, forward(leaf, [rhs[i] for i in range(HALF)], load))
    load.finish()


def both_kernel(place, kept_left, kept_right, inv, rhs, out, left, right, diag, *sems):
    leaf = Leaf(left, right, diag)
    load = Reloader(leaf, place, inv, (kept_left, kept_right), *sems, range(HALF))
    put(out, backward(leaf, forward(leaf, [rhs[i] for i in range(HALF)], load)))


def backward_kernel(place, kept_left, kept_right, inv, rhs, out, left, right, diag, *sems):
    leaf = Leaf(left, right, diag)
    load = Reloader(leaf, place, inv, (kept_left, kept_right), *sems, range(HALF)[::-1])
    put(out, backward(leaf, [rhs[i] for i in range(HALF)], load))


IN_SMEM = pl.BlockSpec(memory_space=pltpu.SMEM)
IN_VMEM = pl.BlockSpec(memory_space=pltpu.VMEM)
IN_HBM = pl.BlockSpec(memory_space=pltpu.HBM)


def limit(mib):
    return pltpu.CompilerParams(vmem_limit_bytes=mib * 1024 * 1024)


def in_hbm(v):
    return pltpu.with_memory_space_constraint(v, pltpu.HBM)


def leaf_scratch(rank, tile):
    return [
        pltpu.VMEM((TILES, rank, tile), BF),
        pltpu.VMEM((TILES, rank, tile), BF),
        pltpu.VMEM((HALF, tile, tile), BF),
    ]


def leaf_sems():
    dma = pltpu.SemaphoreType.DMA
    return [dma((HALF,)), dma((HALF,)), dma((TILES,))]


def load_and_forward(place, tiles, inv, rhs):
    rank, tile = tiles.shape[1] // 2, tiles.shape[2]
    factors = pltpu.HBM((TILES, rank, tile), BF)
    return pl.pallas_call(
        load_kernel,
        out_shape=(jax.ShapeDtypeStruct(rhs.shape, F32), factors, factors),
        in_specs=[IN_SMEM, IN_HBM, IN_HBM, IN_VMEM],
        out_specs=(IN_VMEM, IN_HBM, IN_HBM),
        scratch_shapes=[
            pltpu.VMEM((SLOTS, HALF - 1, 2 * rank, tile), F32),
            *leaf_scratch(rank, tile),
            pltpu.SemaphoreType.DMA((TILES,)),
            *leaf_sems(),
        ],
        compiler_params=limit(36),
    )(place, in_hbm(tiles), in_hbm(inv), rhs)


def solve(body, place, left, right, inv, rhs):
    return pl.pallas_call(
        body,
        out_shape=jax.ShapeDtypeStruct(rhs.shape, F32),
        in_specs=[IN_SMEM, IN_HBM, IN_HBM, IN_HBM, IN_VMEM],
        out_specs=IN_VMEM,
        scratch_shapes=[*leaf_scratch(*left.shape[1:]), *leaf_sems()],
        compiler_params=limit(24),
    )(place, in_hbm(left), in_hbm(right), in_hbm(inv), rhs)


def per_device(
    root_rhs, diag_inv, tile_u, tile_v, tile_rank, child_x, border_t, child_inv, child_blocks
):
    my_row = lax.axis_index(ROW)
    my_col = lax.axis_index(COL)
    ntile = diag_inv.shape[0]
    tile = diag_inv.shape[1]
    rhs_count = root_rhs.shape[0]
    rank_max = tile_u.shape[4]
    n_child = child_x.shape[0]
    nblk = ntile * tile // BLK
    ndev = lax.axis_size(ALL)
    upper = my_row >= HALF
    in_half = my_row % HALF
    half = lax.axis_index("yh")

    left = tile_u[0, 0, 0]
    live = jnp.arange(rank_max)[None, None, :] < tile_rank[0, 0, 0][:, None, None]
    right = jnp.where(live, tile_v[0, 0, 0].astype(F32), 0.0)

    leaf_u = jnp.where(upper, left[1], left[0]).astype(F32)
    leaf_vt = jnp.where(upper, right[1], right[0]).T
    own_tile = with_layout_constraint(jnp.concatenate([leaf_u, leaf_vt], axis=0), ROWS)
    other_tile = lax.ppermute(own_tile, ALL, plane_pairs())
    share = jnp.where(my_col < in_half, own_tile, other_tile)
    share = with_layout_constraint(share, ROWS)
    tiles = lax.all_gather(share, PLANE)
    place = jnp.stack([lax.axis_index("yl"), half]).astype(jnp.int32)

    upward = jnp.einsum("crs,csb->crb", child_x, border_t, preferred_element_type=F32)
    pieces = (
        upward.reshape(n_child, rhs_count, BB, BLK)
        .transpose(1, 0, 2, 3)
        .reshape(rhs_count, n_child * BB, BLK)
    )
    flat_blocks = child_blocks.reshape(-1)
    dense = jnp.zeros((rhs_count, nblk, BLK), F32).at[:, flat_blocks, :].add(pieces)
    width = ntile * tile // ndev
    parts = dense.reshape(rhs_count, ndev, width).transpose(1, 0, 2)
    mine = lax.all_to_all(parts, ALL, split_axis=0, concat_axis=0, tiled=True).sum(axis=0)
    child_sum = copies(mine, ALL).reshape(ndev, rhs_count, width)
    child_sum = child_sum.transpose(1, 0, 2).reshape(rhs_count, ntile, tile).transpose(1, 0, 2)
    rhs = root_rhs.reshape(rhs_count, ntile, tile).transpose(1, 0, 2).astype(F32) - child_sum

    own_rhs = lax.dynamic_slice_in_dim(rhs, HALF * half, HALF, 0)
    x_low, kept_left, kept_right = load_and_forward(place, tiles, diag_inv, own_rhs)
    v0 = right[0].astype(BF)
    u0 = left[0]
    x_col = lax.dynamic_index_in_dim(x_low, my_col, 0, keepdims=False)
    x_own = lax.ppermute(x_col, "yh", [(0, 1)])
    x_own = x_own + jnp.where(upper, 0.0, x_col)
    p = dot_nn(x_own.astype(BF), v0).astype(BF)
    row_sum = copies(dot_nn(p, u0), COL).reshape(8, rhs_count, tile).sum(axis=0)
    row_sums = copies(row_sum, HALF_ROW).reshape(HALF, rhs_count, tile)
    z_high = solve(both_kernel, place, kept_left, kept_right, diag_inv, own_rhs - row_sums)

    z_own = lax.dynamic_index_in_dim(z_high, in_half, 0, keepdims=False).astype(BF)
    q = dot_nt(z_own, u0).astype(BF)
    col_sum = copies(dot_nt(q, v0), HALF_ROW).reshape(HALF, rhs_count, tile).sum(axis=0)
    col_sum = lax.ppermute(col_sum, "yh", [(1, 0)])
    col_sums = copies(col_sum, COL).reshape(8, rhs_count, tile)
    low_rhs = x_low - col_sums
    z_low = solve(backward_kernel, place, kept_left, kept_right, diag_inv, low_rhs)
    z_mine = jnp.where(upper, z_high, z_low)
    z_other = lax.ppermute(z_mine, "yh", [(0, 1), (1, 0)])
    low_part = jnp.where(upper, z_other, z_mine)
    high_part = jnp.where(upper, z_mine, z_other)
    result = jnp.concatenate([low_part, high_part], axis=0).transpose(1, 0, 2)
    result = result.reshape(rhs_count, ntile * tile)

    start = (my_row * 8 + my_col) * width
    root_part = lax.dynamic_slice_in_dim(result, start, width, 1)
    gathered = result.reshape(rhs_count, nblk, BLK)[:, flat_blocks, :]
    gathered = gathered.reshape(rhs_count, n_child, BB * BLK).astype(BF)
    returned = jnp.einsum("rcb,csb->crs", gathered, border_t, preferred_element_type=F32)
    child_out = child_x.astype(F32) - jnp.einsum(
        "crs,cst->crt", returned, child_inv.astype(F32)
    )
    return (root_part, child_out)


def solution(mesh):
    finer = Mesh(mesh.devices.reshape(2, 2, 4, 4, 2), ALL)
    in_specs = (
        P(),
        P(),
        P(ROW, COL, None, None, None, None),
        P(ROW, COL, None, None, None, None),
        P(ROW, COL, None, None),
        P(ALL, None, None),
        P(ALL, None, None),
        P(ALL, None, None),
        P(ALL, None),
    )
    out_specs = (P(None, ALL), P(ALL, None, None))
    return jax.shard_map(
        per_device, mesh=finer, in_specs=in_specs, out_specs=out_specs, check_vma=False
    )
```

```python
import functools

import jax
import jax.numpy as jnp
from jax import lax
from jax.experimental import pallas as pl
from jax.experimental.layout import Layout, with_layout_constraint
from jax.experimental.pallas import tpu as pltpu
from jax.sharding import Mesh
from jax.sharding import PartitionSpec as P

BLK = 128
BB = 8
ROW = ("yh", "yl", "z")
HALF_ROW = ("yl", "z")
COL = ("x", "c")
PLANE = ("z", "x", "c")
ALL = ("yh", "yl", "z", "x", "c")
HALF_ALL = ("yl", "z", "x", "c")
HALF = 8
BF = jnp.bfloat16
F32 = jnp.float32
ROWS = Layout((0, 1))


def copies(v, axis):
    n = lax.axis_size(axis)
    stacked = jnp.broadcast_to(v, (n, *v.shape))
    return lax.all_to_all(stacked, axis, split_axis=0, concat_axis=0, tiled=True)


def dot_nn(a, b):
    return lax.dot_general(a, b, (((1,), (0,)), ((), ())), preferred_element_type=F32)


def dot_nt(a, b):
    return lax.dot_general(a, b, (((1,), (1,)), ((), ())), preferred_element_type=F32)


def exact(dot, a, b):
    high = a.astype(BF)
    low = (a - high.astype(F32)).astype(BF)
    both = dot(jnp.concatenate([high, low], axis=0), b)
    n = a.shape[0]
    return both[:n] + both[n:]


def first_tile(row):
    return row * (row - 1) // 2


SLOTS = 3
TILES = first_tile(HALF)
SPARE = {(1, 0): (1, 7), (2, 0): (2, 6), (2, 1): (2, 7), (3, 0): (0, 6), (3, 1): (3, 7), (3, 2): (0, 7)}


def spot(plane, i, k):
    z = i % 4
    own = i // 4 == plane
    if own or (plane == 0 and k >= z):
        return 8 * z + k
    z, k = SPARE[z, k]
    return 8 * z + k


def plane_pairs():
    pairs = []
    for half in range(2):
        for i in range(HALF):
            for k in range(i):
                plane = i // 4
                source = 64 * half + 32 * plane + spot(plane, i, k)
                target = 64 * half + 32 * (1 - plane) + spot(1 - plane, i, k)
                pairs.append((source, target))
    return pairs


class Leaf:
    def __init__(self, left, right, diag):
        self.left, self.right, self.diag = left, right, diag

    def column(self, j):
        return sum(HALF - 1 - m for m in range(j))

    def u(self, i, k, count=1):
        at = first_tile(i) + k
        return self.left[at : at + count].reshape(-1, self.left.shape[2])

    def vt(self, i, k, count=1):
        at = self.column(k) + i - k - 1
        return self.right[at : at + count].reshape(-1, self.right.shape[2])


class Moves:
    def __init__(self, rows):
        self.rows = rows

    def start(self, i):
        for move in self.rows.get(i, []):
            move.start()

    def wait(self, i):
        for move in self.rows.get(i, []):
            move.wait()


def inverse_moves(leaf, first, inv, sems):
    return Moves(
        {
            n: [pltpu.make_async_copy(inv.at[first + n], leaf.diag.at[n], sems.at[n])]
            for n in range(HALF)
        }
    )


def factor_moves(leaf, kept_left, kept_right, lsems, rsems, keep):
    rows = {}
    for i in range(1, HALF):
        at = first_tile(i)
        pairs = [(kept_left.at[pl.ds(at, i)], leaf.left.at[pl.ds(at, i)], lsems.at[i])]
        for k in range(i):
            place = leaf.column(k) + i - k - 1
            pairs.append((kept_right.at[place], leaf.right.at[place], rsems.at[place]))
        rows[i] = [
            pltpu.make_async_copy(*((b, a) if keep else (a, b)), sem) for a, b, sem in pairs
        ]
    return Moves(rows)


class Loader:
    def __init__(self, leaf, place, tiles, inv, kept, stage, sems, dsems, lsems, rsems):
        self.leaf, self.stage = leaf, stage
        rows = {}
        for i in range(1, HALF):
            rows[i] = []
            for k in range(i):
                one, two = spot(0, i, k), spot(1, i, k)
                rows[i].append(
                    pltpu.make_async_copy(
                        tiles.at[one + place[0] * (two - one)],
                        stage.at[i % SLOTS, k],
                        sems.at[first_tile(i) + k],
                    )
                )
        self.tiles = Moves(rows)
        self.inverse = inverse_moves(leaf, HALF * place[1], inv, dsems)
        self.kept = factor_moves(leaf, *kept, lsems, rsems, True)
        for i in range(SLOTS):
            self.start(i)
        self(0)

    def start(self, i):
        self.inverse.start(i)
        self.tiles.start(i)

    def __call__(self, i):
        leaf = self.leaf
        rank = leaf.left.shape[1]
        self.inverse.wait(i)
        self.tiles.wait(i)
        for k in range(i):
            leaf.left[first_tile(i) + k] = self.stage[i % SLOTS, k, :rank].astype(BF)
            leaf.right[leaf.column(k) + i - k - 1] = self.stage[i % SLOTS, k, rank:].astype(BF)
        self.kept.start(i - 1)
        if i + SLOTS < HALF:
            self.start(i + SLOTS)

    def finish(self):
        self.kept.start(HALF - 1)
        for i in range(HALF):
            self.kept.wait(i)


class Reloader:
    def __init__(self, leaf, place, inv, kept, dsems, lsems, rsems, order):
        self.inverse = inverse_moves(leaf, HALF * place[1], inv, dsems)
        self.factors = factor_moves(leaf, *kept, lsems, rsems, False)
        for i in order:
            self.inverse.start(i)
            self.factors.start(i)
        self(order[0])

    def __call__(self, i):
        self.inverse.wait(i)
        self.factors.wait(i)


def forward(leaf, rhs, load=None):
    solved, narrow = [], []
    partial = rhs[0]
    last = None
    for i in range(HALF):
        acc = partial
        if i:
            acc = acc - dot_nn(last, leaf.u(i, i - 1))
        x = exact(dot_nn, acc, leaf.diag[i])
        if i + 1 < HALF:
            if load:
                load(i + 1)
            partial = rhs[i + 1]
            if i:
                known = [dot_nt(narrow[k], leaf.vt(i + 1, k)).astype(BF) for k in range(i)]
                partial = partial - dot_nn(jnp.concatenate(known, axis=1), leaf.u(i + 1, 0, i))
        solved.append(x)
        narrow.append(x.astype(BF))
        if i + 1 < HALF:
            last = dot_nt(narrow[i], leaf.vt(i + 1, i)).astype(BF)
    return solved


def backward(leaf, rhs, load=None):
    width = leaf.left.shape[1]
    solved = [None] * HALF
    waiting = {j: [] for j in range(HALF)}
    partial = rhs[HALF - 1]
    last = None
    for j in reversed(range(HALF)):
        acc = partial
        if j + 1 < HALF:
            acc = acc - dot_nn(last, leaf.vt(j + 1, j))
        z = exact(dot_nt, acc, leaf.diag[j])
        if j:
            if load:
                load(j - 1)
            partial = rhs[j - 1]
            if waiting[j - 1]:
                known = jnp.concatenate(waiting[j - 1][::-1], axis=1)
                partial = partial - dot_nn(known, leaf.vt(j + 1, j - 1, HALF - 1 - j))
        solved[j] = z
        narrow = z.astype(BF)
        if j:
            last = dot_nt(narrow, leaf.u(j, j - 1)).astype(BF)
        if j > 1:
            others = dot_nt(narrow, leaf.u(j, 0, j - 1)).astype(BF)
            for k in range(j - 1):
                waiting[k].append(others[:, k * width : (k + 1) * width])
    return solved


def put(out, values):
    for i in range(HALF):
        out[i] = values[i]


def load_kernel(place, tiles, inv, rhs, out, kept_left, kept_right, stage, *scratch):
    left, right, diag, sems, dsems, lsems, rsems = scratch
    leaf = Leaf(left, right, diag)
    kept = (kept_left, kept_right)
    load = Loader(leaf, place, tiles, inv, kept, stage, sems, dsems, lsems, rsems)
    put(out, forward(leaf, [rhs[i] for i in range(HALF)], load))
    load.finish()


def both_kernel(place, kept_left, kept_right, inv, rhs, out, left, right, diag, *sems):
    leaf = Leaf(left, right, diag)
    load = Reloader(leaf, place, inv, (kept_left, kept_right), *sems, range(HALF))
    put(out, backward(leaf, forward(leaf, [rhs[i] for i in range(HALF)], load)))


def backward_kernel(place, kept_left, kept_right, inv, rhs, out, left, right, diag, *sems):
    leaf = Leaf(left, right, diag)
    load = Reloader(leaf, place, inv, (kept_left, kept_right), *sems, range(HALF)[::-1])
    put(out, backward(leaf, [rhs[i] for i in range(HALF)], load))


IN_SMEM = pl.BlockSpec(memory_space=pltpu.SMEM)
IN_VMEM = pl.BlockSpec(memory_space=pltpu.VMEM)
IN_HBM = pl.BlockSpec(memory_space=pltpu.HBM)


def limit(mib):
    return pltpu.CompilerParams(vmem_limit_bytes=mib * 1024 * 1024)


def in_hbm(v):
    return pltpu.with_memory_space_constraint(v, pltpu.HBM)


def leaf_scratch(rank, tile):
    return [
        pltpu.VMEM((TILES, rank, tile), BF),
        pltpu.VMEM((TILES, rank, tile), BF),
        pltpu.VMEM((HALF, tile, tile), BF),
    ]


def leaf_sems():
    dma = pltpu.SemaphoreType.DMA
    return [dma((HALF,)), dma((HALF,)), dma((TILES,))]


def load_and_forward(place, tiles, inv, rhs):
    rank, tile = tiles.shape[1] // 2, tiles.shape[2]
    factors = pltpu.HBM((TILES, rank, tile), BF)
    return pl.pallas_call(
        load_kernel,
        out_shape=(jax.ShapeDtypeStruct(rhs.shape, F32), factors, factors),
        in_specs=[IN_SMEM, IN_HBM, IN_HBM, IN_VMEM],
        out_specs=(IN_VMEM, IN_HBM, IN_HBM),
        scratch_shapes=[
            pltpu.VMEM((SLOTS, HALF - 1, 2 * rank, tile), F32),
            *leaf_scratch(rank, tile),
            pltpu.SemaphoreType.DMA((TILES,)),
            *leaf_sems(),
        ],
        compiler_params=limit(36),
    )(place, in_hbm(tiles), in_hbm(inv), rhs)


def solve(body, place, left, right, inv, rhs):
    return pl.pallas_call(
        body,
        out_shape=jax.ShapeDtypeStruct(rhs.shape, F32),
        in_specs=[IN_SMEM, IN_HBM, IN_HBM, IN_HBM, IN_VMEM],
        out_specs=IN_VMEM,
        scratch_shapes=[*leaf_scratch(*left.shape[1:]), *leaf_sems()],
        compiler_params=limit(24),
    )(place, in_hbm(left), in_hbm(right), in_hbm(inv), rhs)


def per_device(
    root_rhs, diag_inv, tile_u, tile_v, tile_rank, child_x, border_t, child_inv, child_blocks
):
    my_row = lax.axis_index(ROW)
    my_col = lax.axis_index(COL)
    ntile = diag_inv.shape[0]
    tile = diag_inv.shape[1]
    rhs_count = root_rhs.shape[0]
    rank_max = tile_u.shape[4]
    n_child = child_x.shape[0]
    nblk = ntile * tile // BLK
    ndev = lax.axis_size(ALL)
    upper = my_row >= HALF
    in_half = my_row % HALF
    half = lax.axis_index("yh")

    left = tile_u[0, 0, 0]
    live = jnp.arange(rank_max)[None, None, :] < tile_rank[0, 0, 0][:, None, None]
    right = jnp.where(live, tile_v[0, 0, 0].astype(F32), 0.0)

    leaf_u = jnp.where(upper, left[1], left[0]).astype(F32)
    leaf_vt = jnp.where(upper, right[1], right[0]).T
    own_tile = with_layout_constraint(jnp.concatenate([leaf_u, leaf_vt], axis=0), ROWS)
    other_tile = lax.ppermute(own_tile, ALL, plane_pairs())
    upward = jnp.einsum("crs,csb->crb", child_x, border_t, preferred_element_type=F32)
    pieces = (
        upward.reshape(n_child, rhs_count, BB, BLK)
        .transpose(1, 0, 2, 3)
        .reshape(rhs_count, n_child * BB, BLK)
    )
    flat_blocks = child_blocks.reshape(-1)
    dense = jnp.zeros((rhs_count, nblk, BLK), F32).at[:, flat_blocks, :].add(pieces)
    width = ntile * tile // ndev
    parts = dense.reshape(rhs_count, ndev, width).transpose(1, 0, 2)
    mine = lax.all_to_all(parts, ALL, split_axis=0, concat_axis=0, tiled=True).sum(axis=0)
    other_tile, mine = lax.optimization_barrier((other_tile, mine))
    share = jnp.where(my_col < in_half, own_tile, other_tile)
    share = with_layout_constraint(share, ROWS)
    tiles = lax.all_gather(share, PLANE)
    place = jnp.stack([lax.axis_index("yl"), half]).astype(jnp.int32)
    child_sum = copies(mine, HALF_ALL).reshape(ndev // 2, rhs_count, width)
    child_sum = child_sum.transpose(1, 0, 2).reshape(rhs_count, HALF, tile).transpose(1, 0, 2)
    given = root_rhs.reshape(rhs_count, ntile, tile)
    given = lax.dynamic_slice_in_dim(given, HALF * half, HALF, 1)
    own_rhs = given.transpose(1, 0, 2).astype(F32) - child_sum

    x_low, kept_left, kept_right = load_and_forward(place, tiles, diag_inv, own_rhs)
    v0 = right[0].astype(BF)
    u0 = left[0]
    x_col = lax.dynamic_index_in_dim(x_low, my_col, 0, keepdims=False)
    x_own = lax.ppermute(x_col, "yh", [(0, 1)])
    x_own = x_own + jnp.where(upper, 0.0, x_col)
    p = dot_nn(x_own.astype(BF), v0).astype(BF)
    row_sum = copies(dot_nn(p, u0), COL).reshape(8, rhs_count, tile).sum(axis=0)
    row_sums = copies(row_sum, HALF_ROW).reshape(HALF, rhs_count, tile)
    z_high = solve(both_kernel, place, kept_left, kept_right, diag_inv, own_rhs - row_sums)

    z_own = lax.dynamic_index_in_dim(z_high, in_half, 0, keepdims=False).astype(BF)
    q = dot_nt(z_own, u0).astype(BF)
    col_sum = copies(dot_nt(q, v0), HALF_ROW).reshape(HALF, rhs_count, tile).sum(axis=0)
    col_sum = lax.ppermute(col_sum, "yh", [(1, 0)])
    col_sums = copies(col_sum, COL).reshape(8, rhs_count, tile)
    low_rhs = x_low - col_sums
    z_low = solve(backward_kernel, place, kept_left, kept_right, diag_inv, low_rhs)
    z_mine = jnp.where(upper, z_high, z_low)
    z_other = lax.ppermute(z_mine, "yh", [(0, 1), (1, 0)])
    low_part = jnp.where(upper, z_other, z_mine)
    high_part = jnp.where(upper, z_mine, z_other)
    result = jnp.concatenate([low_part, high_part], axis=0).transpose(1, 0, 2)
    result = result.reshape(rhs_count, ntile * tile)

    start = (my_row * 8 + my_col) * width
    root_part = lax.dynamic_slice_in_dim(result, start, width, 1)
    gathered = result.reshape(rhs_count, nblk, BLK)[:, flat_blocks, :]
    gathered = gathered.reshape(rhs_count, n_child, BB * BLK).astype(BF)
    returned = jnp.einsum("rcb,csb->crs", gathered, border_t, preferred_element_type=F32)
    child_out = child_x.astype(F32) - jnp.einsum(
        "crs,cst->crt", returned, child_inv.astype(F32)
    )
    return (root_part, child_out)


def solution(mesh):
    finer = Mesh(mesh.devices.reshape(2, 2, 4, 4, 2), ALL)
    in_specs = (
        P(),
        P(),
        P(ROW, COL, None, None, None, None),
        P(ROW, COL, None, None, None, None),
        P(ROW, COL, None, None),
        P(ALL, None, None),
        P(ALL, None, None),
        P(ALL, None, None),
        P(ALL, None),
    )
    out_specs = (P(None, ALL), P(ALL, None, None))
    return jax.shard_map(
        per_device, mesh=finer, in_specs=in_specs, out_specs=out_specs, check_vma=False
    )
```

```python
import jax
import jax.numpy as jnp
from jax import lax
from jax.experimental import pallas as pl
from jax.experimental.layout import Layout, with_layout_constraint
from jax.experimental.pallas import tpu as pltpu
from jax.sharding import Mesh
from jax.sharding import PartitionSpec as P

BLK = 128
BB = 8
ROW = ("yh", "yl", "z")
HALF_ROW = ("yl", "z")
COL = ("x", "c")
PLANE = ("z", "x", "c")
ALL = ("yh", "yl", "z", "x", "c")
HALF_ALL = ("yl", "z", "x", "c")
HALF = 8
BF = jnp.bfloat16
F32 = jnp.float32
ROWS = Layout((0, 1))


def copies(v, axis):
    n = lax.axis_size(axis)
    stacked = jnp.broadcast_to(v, (n, *v.shape))
    return lax.all_to_all(stacked, axis, split_axis=0, concat_axis=0, tiled=True)


def dot_nn(a, b):
    return lax.dot_general(a, b, (((1,), (0,)), ((), ())), preferred_element_type=F32)


def dot_nt(a, b):
    return lax.dot_general(a, b, (((1,), (1,)), ((), ())), preferred_element_type=F32)


def exact(dot, a, b):
    high = a.astype(BF)
    low = (a - high.astype(F32)).astype(BF)
    both = dot(jnp.concatenate([high, low], axis=0), b)
    n = a.shape[0]
    return both[:n] + both[n:]


def first_tile(row):
    return row * (row - 1) // 2


SLOTS = 3
TILES = first_tile(HALF)
SPARE = {(1, 0): (1, 7), (2, 0): (2, 6), (2, 1): (2, 7), (3, 0): (0, 6), (3, 1): (3, 7), (3, 2): (0, 7)}


def spot(plane, i, k):
    z = i % 4
    own = i // 4 == plane
    if own or (plane == 0 and k >= z):
        return 8 * z + k
    z, k = SPARE[z, k]
    return 8 * z + k


def plane_pairs():
    pairs = []
    for half in range(2):
        for i in range(HALF):
            for k in range(i):
                plane = i // 4
                source = 64 * half + 32 * plane + spot(plane, i, k)
                target = 64 * half + 32 * (1 - plane) + spot(1 - plane, i, k)
                pairs.append((source, target))
    return pairs


class Leaf:
    def __init__(self, left, right, diag):
        self.left, self.right, self.diag = left, right, diag

    def column(self, j):
        return sum(HALF - 1 - m for m in range(j))

    def u(self, i, k, count=1):
        at = first_tile(i) + k
        return self.left[at : at + count].reshape(-1, self.left.shape[2])

    def vt(self, i, k, count=1):
        at = self.column(k) + i - k - 1
        return self.right[at : at + count].reshape(-1, self.right.shape[2])


class Moves:
    def __init__(self, rows):
        self.rows = rows

    def start(self, i):
        for move in self.rows.get(i, []):
            move.start()

    def wait(self, i):
        for move in self.rows.get(i, []):
            move.wait()


def inverse_moves(leaf, first, inv, sems):
    return Moves(
        {
            n: [pltpu.make_async_copy(inv.at[first + n], leaf.diag.at[n], sems.at[n])]
            for n in range(HALF)
        }
    )


def factor_moves(leaf, kept_left, kept_right, lsems, rsems, keep):
    rows = {}
    for i in range(1, HALF):
        at = first_tile(i)
        pairs = [(kept_left.at[pl.ds(at, i)], leaf.left.at[pl.ds(at, i)], lsems.at[i])]
        for k in range(i):
            place = leaf.column(k) + i - k - 1
            pairs.append((kept_right.at[place], leaf.right.at[place], rsems.at[place]))
        rows[i] = [
            pltpu.make_async_copy(*((b, a) if keep else (a, b)), sem) for a, b, sem in pairs
        ]
    return Moves(rows)


class Loader:
    def __init__(self, leaf, place, tiles, inv, kept, stage, sems, dsems, lsems, rsems):
        self.leaf, self.stage = leaf, stage
        rows = {}
        for i in range(1, HALF):
            rows[i] = []
            for k in range(i):
                one, two = spot(0, i, k), spot(1, i, k)
                rows[i].append(
                    pltpu.make_async_copy(
                        tiles.at[one + place[0] * (two - one)],
                        stage.at[i % SLOTS, k],
                        sems.at[first_tile(i) + k],
                    )
                )
        self.tiles = Moves(rows)
        self.inverse = inverse_moves(leaf, HALF * place[1], inv, dsems)
        self.kept = factor_moves(leaf, *kept, lsems, rsems, True)
        for i in range(SLOTS):
            self.start(i)
        self(0)

    def start(self, i):
        self.inverse.start(i)
        self.tiles.start(i)

    def __call__(self, i):
        leaf = self.leaf
        rank = leaf.left.shape[1]
        self.inverse.wait(i)
        self.tiles.wait(i)
        for k in range(i):
            leaf.left[first_tile(i) + k] = self.stage[i % SLOTS, k, :rank].astype(BF)
            leaf.right[leaf.column(k) + i - k - 1] = self.stage[i % SLOTS, k, rank:].astype(BF)
        self.kept.start(i - 1)
        if i + SLOTS < HALF:
            self.start(i + SLOTS)

    def finish(self):
        self.kept.start(HALF - 1)
        for i in range(HALF):
            self.kept.wait(i)


class Reloader:
    def __init__(self, leaf, place, inv, kept, dsems, lsems, rsems, order):
        self.inverse = inverse_moves(leaf, HALF * place[1], inv, dsems)
        self.factors = factor_moves(leaf, *kept, lsems, rsems, False)
        for i in order:
            self.inverse.start(i)
            self.factors.start(i)
        self(order[0])

    def __call__(self, i):
        self.inverse.wait(i)
        self.factors.wait(i)


def forward(leaf, rhs, load=None):
    solved, narrow = [], []
    partial = rhs[0]
    last = None
    for i in range(HALF):
        acc = partial
        if i:
            acc = acc - dot_nn(last, leaf.u(i, i - 1))
        x = exact(dot_nn, acc, leaf.diag[i])
        if i + 1 < HALF:
            if load:
                load(i + 1)
            partial = rhs[i + 1]
            if i:
                known = [dot_nt(narrow[k], leaf.vt(i + 1, k)).astype(BF) for k in range(i)]
                partial = partial - dot_nn(jnp.concatenate(known, axis=1), leaf.u(i + 1, 0, i))
        solved.append(x)
        narrow.append(x.astype(BF))
        if i + 1 < HALF:
            last = dot_nt(narrow[i], leaf.vt(i + 1, i)).astype(BF)
    return solved


def backward(leaf, rhs, load=None):
    width = leaf.left.shape[1]
    solved = [None] * HALF
    waiting = {j: [] for j in range(HALF)}
    partial = rhs[HALF - 1]
    last = None
    for j in reversed(range(HALF)):
        acc = partial
        if j + 1 < HALF:
            acc = acc - dot_nn(last, leaf.vt(j + 1, j))
        z = exact(dot_nt, acc, leaf.diag[j])
        if j:
            if load:
                load(j - 1)
            partial = rhs[j - 1]
            if waiting[j - 1]:
                known = jnp.concatenate(waiting[j - 1][::-1], axis=1)
                partial = partial - dot_nn(known, leaf.vt(j + 1, j - 1, HALF - 1 - j))
        solved[j] = z
        narrow = z.astype(BF)
        if j:
            last = dot_nt(narrow, leaf.u(j, j - 1)).astype(BF)
        if j > 1:
            others = dot_nt(narrow, leaf.u(j, 0, j - 1)).astype(BF)
            for k in range(j - 1):
                waiting[k].append(others[:, k * width : (k + 1) * width])
    return solved


def put(out, values):
    for i in range(HALF):
        out[i] = values[i]


def load_kernel(place, tiles, inv, rhs, out, kept_left, kept_right, stage, *scratch):
    left, right, diag, sems, dsems, lsems, rsems = scratch
    leaf = Leaf(left, right, diag)
    kept = (kept_left, kept_right)
    load = Loader(leaf, place, tiles, inv, kept, stage, sems, dsems, lsems, rsems)
    put(out, forward(leaf, [rhs[i] for i in range(HALF)], load))
    load.finish()


def both_kernel(place, kept_left, kept_right, inv, rhs, out, left, right, diag, *sems):
    leaf = Leaf(left, right, diag)
    load = Reloader(leaf, place, inv, (kept_left, kept_right), *sems, range(HALF))
    put(out, backward(leaf, forward(leaf, [rhs[i] for i in range(HALF)], load)))


def backward_kernel(place, kept_left, kept_right, inv, rhs, out, left, right, diag, *sems):
    leaf = Leaf(left, right, diag)
    load = Reloader(leaf, place, inv, (kept_left, kept_right), *sems, range(HALF)[::-1])
    put(out, backward(leaf, [rhs[i] for i in range(HALF)], load))


IN_SMEM = pl.BlockSpec(memory_space=pltpu.SMEM)
IN_VMEM = pl.BlockSpec(memory_space=pltpu.VMEM)
IN_HBM = pl.BlockSpec(memory_space=pltpu.HBM)


def limit(mib):
    return pltpu.CompilerParams(vmem_limit_bytes=mib * 1024 * 1024)


def in_hbm(v):
    return pltpu.with_memory_space_constraint(v, pltpu.HBM)


def leaf_scratch(rank, tile):
    return [
        pltpu.VMEM((TILES, rank, tile), BF),
        pltpu.VMEM((TILES, rank, tile), BF),
        pltpu.VMEM((HALF, tile, tile), BF),
    ]


def leaf_sems():
    dma = pltpu.SemaphoreType.DMA
    return [dma((HALF,)), dma((HALF,)), dma((TILES,))]


def load_and_forward(place, tiles, inv, rhs):
    rank, tile = tiles.shape[1] // 2, tiles.shape[2]
    factors = pltpu.HBM((TILES, rank, tile), BF)
    return pl.pallas_call(
        load_kernel,
        out_shape=(jax.ShapeDtypeStruct(rhs.shape, F32), factors, factors),
        in_specs=[IN_SMEM, IN_HBM, IN_HBM, IN_VMEM],
        out_specs=(IN_VMEM, IN_HBM, IN_HBM),
        scratch_shapes=[
            pltpu.VMEM((SLOTS, HALF - 1, 2 * rank, tile), F32),
            *leaf_scratch(rank, tile),
            pltpu.SemaphoreType.DMA((TILES,)),
            *leaf_sems(),
        ],
        compiler_params=limit(36),
    )(place, in_hbm(tiles), in_hbm(inv), rhs)


def solve(body, place, left, right, inv, rhs):
    return pl.pallas_call(
        body,
        out_shape=jax.ShapeDtypeStruct(rhs.shape, F32),
        in_specs=[IN_SMEM, IN_HBM, IN_HBM, IN_HBM, IN_VMEM],
        out_specs=IN_VMEM,
        scratch_shapes=[*leaf_scratch(*left.shape[1:]), *leaf_sems()],
        compiler_params=limit(24),
    )(place, in_hbm(left), in_hbm(right), in_hbm(inv), rhs)


def per_device(
    root_rhs, diag_inv, tile_u, tile_v, tile_rank, child_x, border_t, child_inv, child_blocks
):
    my_row = lax.axis_index(ROW)
    my_col = lax.axis_index(COL)
    ntile = diag_inv.shape[0]
    tile = diag_inv.shape[1]
    rhs_count = root_rhs.shape[0]
    rank_max = tile_u.shape[4]
    n_child = child_x.shape[0]
    nblk = ntile * tile // BLK
    ndev = lax.axis_size(ALL)
    upper = my_row >= HALF
    in_half = my_row % HALF
    half = lax.axis_index("yh")

    left = tile_u[0, 0, 0]
    live = jnp.arange(rank_max)[None, None, :] < tile_rank[0, 0, 0][:, None, None]
    right = jnp.where(live, tile_v[0, 0, 0].astype(F32), 0.0)

    leaf_u = jnp.where(upper, left[1], left[0]).astype(F32)
    leaf_vt = jnp.where(upper, right[1], right[0]).T
    own_tile = with_layout_constraint(jnp.concatenate([leaf_u, leaf_vt], axis=0), ROWS)
    other_tile = lax.ppermute(own_tile, ALL, plane_pairs())
    upward = jnp.einsum("crs,csb->crb", child_x, border_t, preferred_element_type=F32)
    pieces = (
        upward.reshape(n_child, rhs_count, BB, BLK)
        .transpose(1, 0, 2, 3)
        .reshape(rhs_count, n_child * BB, BLK)
    )
    flat_blocks = child_blocks.reshape(-1)
    dense = jnp.zeros((rhs_count, nblk, BLK), F32).at[:, flat_blocks, :].add(pieces)
    width = ntile * tile // ndev
    parts = dense.reshape(rhs_count, ndev, width).transpose(1, 0, 2)
    mine = lax.all_to_all(parts, ALL, split_axis=0, concat_axis=0, tiled=True)
    mine = mine.sum(axis=0)
    share = jnp.where(my_col < in_half, own_tile, other_tile)
    share = with_layout_constraint(share, ROWS)
    tiles = lax.all_gather(share, PLANE)
    place = jnp.stack([lax.axis_index("yl"), half]).astype(jnp.int32)
    child_sum = copies(mine, HALF_ALL).reshape(ndev // 2, rhs_count, width)
    child_sum = child_sum.transpose(1, 0, 2).reshape(rhs_count, HALF, tile).transpose(1, 0, 2)
    given = root_rhs.reshape(rhs_count, ntile, tile)
    given = lax.dynamic_slice_in_dim(given, HALF * half, HALF, 1)
    own_rhs = given.transpose(1, 0, 2).astype(F32) - child_sum

    x_low, kept_left, kept_right = load_and_forward(place, tiles, diag_inv, own_rhs)
    v0 = right[0].astype(BF)
    u0 = left[0]
    x_col = lax.dynamic_index_in_dim(x_low, my_col, 0, keepdims=False)
    x_own = lax.ppermute(x_col, "yh", [(0, 1)])
    x_own = x_own + jnp.where(upper, 0.0, x_col)
    p = dot_nn(x_own.astype(BF), v0).astype(BF)
    row_sum = copies(dot_nn(p, u0), COL).reshape(8, rhs_count, tile).sum(axis=0)
    row_sums = copies(row_sum, HALF_ROW).reshape(HALF, rhs_count, tile)
    z_high = solve(both_kernel, place, kept_left, kept_right, diag_inv, own_rhs - row_sums)

    z_own = lax.dynamic_index_in_dim(z_high, in_half, 0, keepdims=False).astype(BF)
    q = dot_nt(z_own, u0).astype(BF)
    col_sum = copies(dot_nt(q, v0), HALF_ROW).reshape(HALF, rhs_count, tile).sum(axis=0)
    col_sum = lax.ppermute(col_sum, "yh", [(1, 0)])
    col_sums = copies(col_sum, COL).reshape(8, rhs_count, tile)
    low_rhs = x_low - col_sums
    z_low = solve(backward_kernel, place, kept_left, kept_right, diag_inv, low_rhs)
    z_mine = jnp.where(upper, z_high, z_low)
    z_other = lax.ppermute(z_mine, "yh", [(0, 1), (1, 0)])
    low_part = jnp.where(upper, z_other, z_mine)
    high_part = jnp.where(upper, z_mine, z_other)
    result = jnp.concatenate([low_part, high_part], axis=0).transpose(1, 0, 2)
    result = result.reshape(rhs_count, ntile * tile)

    start = (my_row * 8 + my_col) * width
    root_part = lax.dynamic_slice_in_dim(result, start, width, 1)
    gathered = result.reshape(rhs_count, nblk, BLK)[:, flat_blocks, :]
    gathered = gathered.reshape(rhs_count, n_child, BB * BLK).astype(BF)
    returned = jnp.einsum("rcb,csb->crs", gathered, border_t, preferred_element_type=F32)
    child_out = child_x.astype(F32) - jnp.einsum(
        "crs,cst->crt", returned, child_inv.astype(F32)
    )
    return (root_part, child_out)


def solution(mesh):
    finer = Mesh(mesh.devices.reshape(2, 2, 4, 4, 2), ALL)
    in_specs = (
        P(),
        P(),
        P(ROW, COL, None, None, None, None),
        P(ROW, COL, None, None, None, None),
        P(ROW, COL, None, None),
        P(ALL, None, None),
        P(ALL, None, None),
        P(ALL, None, None),
        P(ALL, None),
    )
    out_specs = (P(None, ALL), P(ALL, None, None))
    return jax.shard_map(
        per_device, mesh=finer, in_specs=in_specs, out_specs=out_specs, check_vma=False
    )
```

```python
import jax
import jax.numpy as jnp
from jax import lax
from jax.experimental import pallas as pl
from jax.experimental.layout import Layout, with_layout_constraint
from jax.experimental.pallas import tpu as pltpu
from jax.sharding import Mesh
from jax.sharding import PartitionSpec as P

BLK = 128
BB = 8
ROW = ("yh", "yl", "z")
HALF_ROW = ("yl", "z")
COL = ("x", "c")
PLANE = ("z", "x", "c")
ALL = ("yh", "yl", "z", "x", "c")
HALF_ALL = ("yl", "z", "x", "c")
HALF = 8
BF = jnp.bfloat16
F32 = jnp.float32
ROWS = Layout((0, 1))


def copies(v, axis):
    n = lax.axis_size(axis)
    stacked = jnp.broadcast_to(v, (n, *v.shape))
    return lax.all_to_all(stacked, axis, split_axis=0, concat_axis=0, tiled=True)


def dot_nn(a, b):
    return lax.dot_general(a, b, (((1,), (0,)), ((), ())), preferred_element_type=F32)


def dot_nt(a, b):
    return lax.dot_general(a, b, (((1,), (1,)), ((), ())), preferred_element_type=F32)


def exact(dot, a, b):
    high = a.astype(BF)
    low = (a - high.astype(F32)).astype(BF)
    both = dot(jnp.concatenate([high, low], axis=0), b)
    n = a.shape[0]
    return both[:n] + both[n:]


def first_tile(row):
    return row * (row - 1) // 2


SLOTS = 3
TILES = first_tile(HALF)
SPARE = {(1, 0): (1, 7), (2, 0): (2, 6), (2, 1): (2, 7), (3, 0): (0, 6), (3, 1): (3, 7), (3, 2): (0, 7)}


def spot(plane, i, k):
    z = i % 4
    own = i // 4 == plane
    if own or (plane == 0 and k >= z):
        return 8 * z + k
    z, k = SPARE[z, k]
    return 8 * z + k


def plane_pairs():
    pairs = []
    for half in range(2):
        for i in range(HALF):
            for k in range(i):
                plane = i // 4
                source = 64 * half + 32 * plane + spot(plane, i, k)
                target = 64 * half + 32 * (1 - plane) + spot(1 - plane, i, k)
                pairs.append((source, target))
    return pairs


class Leaf:
    def __init__(self, left, right, diag):
        self.left, self.right, self.diag = left, right, diag

    def column(self, j):
        return sum(HALF - 1 - m for m in range(j))

    def u(self, i, k, count=1):
        at = first_tile(i) + k
        return self.left[at : at + count].reshape(-1, self.left.shape[2])

    def vt(self, i, k, count=1):
        at = self.column(k) + i - k - 1
        return self.right[at : at + count].reshape(-1, self.right.shape[2])


class Moves:
    def __init__(self, rows):
        self.rows = rows

    def start(self, i):
        for move in self.rows.get(i, []):
            move.start()

    def wait(self, i):
        for move in self.rows.get(i, []):
            move.wait()


def inverse_moves(leaf, first, inv, sems):
    return Moves(
        {
            n: [pltpu.make_async_copy(inv.at[first + n], leaf.diag.at[n], sems.at[n])]
            for n in range(HALF)
        }
    )


def factor_moves(leaf, kept_left, kept_right, lsems, rsems, keep):
    rows = {}
    for i in range(1, HALF):
        at = first_tile(i)
        pairs = [(kept_left.at[pl.ds(at, i)], leaf.left.at[pl.ds(at, i)], lsems.at[i])]
        for k in range(i):
            place = leaf.column(k) + i - k - 1
            pairs.append((kept_right.at[place], leaf.right.at[place], rsems.at[place]))
        rows[i] = [
            pltpu.make_async_copy(*((b, a) if keep else (a, b)), sem) for a, b, sem in pairs
        ]
    return Moves(rows)


class Loader:
    def __init__(self, leaf, place, tiles, inv, kept, stage, sems, dsems, lsems, rsems):
        self.leaf, self.stage = leaf, stage
        rows = {}
        for i in range(1, HALF):
            rows[i] = []
            for k in range(i):
                one, two = spot(0, i, k), spot(1, i, k)
                rows[i].append(
                    pltpu.make_async_copy(
                        tiles.at[one + place[0] * (two - one)],
                        stage.at[i % SLOTS, k],
                        sems.at[first_tile(i) + k],
                    )
                )
        self.tiles = Moves(rows)
        self.inverse = inverse_moves(leaf, HALF * place[1], inv, dsems)
        self.kept = factor_moves(leaf, *kept, lsems, rsems, True)
        for i in range(SLOTS):
            self.start(i)
        self(0)

    def start(self, i):
        self.inverse.start(i)
        self.tiles.start(i)

    def __call__(self, i):
        leaf = self.leaf
        rank = leaf.left.shape[1]
        self.inverse.wait(i)
        self.tiles.wait(i)
        for k in range(i):
            leaf.left[first_tile(i) + k] = self.stage[i % SLOTS, k, :rank].astype(BF)
            leaf.right[leaf.column(k) + i - k - 1] = self.stage[i % SLOTS, k, rank:].astype(BF)
        self.kept.start(i - 1)
        if i + SLOTS < HALF:
            self.start(i + SLOTS)

    def finish(self):
        self.kept.start(HALF - 1)
        for i in range(HALF):
            self.kept.wait(i)


class Reloader:
    def __init__(self, leaf, place, inv, kept, dsems, lsems, rsems, order):
        self.inverse = inverse_moves(leaf, HALF * place[1], inv, dsems)
        self.factors = factor_moves(leaf, *kept, lsems, rsems, False)
        for i in order:
            self.inverse.start(i)
            self.factors.start(i)
        self(order[0])

    def __call__(self, i):
        self.inverse.wait(i)
        self.factors.wait(i)


def forward(leaf, rhs, load=None):
    solved, narrow = [], []
    partial = rhs[0]
    last = None
    for i in range(HALF):
        following = None
        if i + 1 < HALF:
            if load:
                load(i + 1)
            folded = dot_nt(leaf.vt(i + 1, i), leaf.diag[i]).astype(BF)
            following = rhs[i + 1]
            if i:
                known = [dot_nt(narrow[k], leaf.vt(i + 1, k)).astype(BF) for k in range(i)]
                following = following - dot_nn(jnp.concatenate(known, axis=1), leaf.u(i + 1, 0, i))
        acc = partial
        if i:
            acc = acc - dot_nn(last, leaf.u(i, i - 1))
        if i + 1 < HALF:
            last = dot_nt(acc.astype(BF), folded).astype(BF)
        x = exact(dot_nn, acc, leaf.diag[i])
        solved.append(x)
        narrow.append(x.astype(BF))
        partial = following
    return solved


def backward(leaf, rhs, load=None):
    width = leaf.left.shape[1]
    solved = [None] * HALF
    waiting = {j: [] for j in range(HALF)}
    partial = rhs[HALF - 1]
    last = None
    for j in reversed(range(HALF)):
        following = None
        if j:
            if load:
                load(j - 1)
            folded = dot_nn(leaf.u(j, j - 1), leaf.diag[j]).astype(BF)
            following = rhs[j - 1]
            if waiting[j - 1]:
                known = jnp.concatenate(waiting[j - 1][::-1], axis=1)
                following = following - dot_nn(known, leaf.vt(j + 1, j - 1, HALF - 1 - j))
        acc = partial
        if j + 1 < HALF:
            acc = acc - dot_nn(last, leaf.vt(j + 1, j))
        if j:
            last = dot_nt(acc.astype(BF), folded).astype(BF)
        z = exact(dot_nt, acc, leaf.diag[j])
        solved[j] = z
        if j > 1:
            others = dot_nt(z.astype(BF), leaf.u(j, 0, j - 1)).astype(BF)
            for k in range(j - 1):
                waiting[k].append(others[:, k * width : (k + 1) * width])
        partial = following
    return solved


def put(out, values):
    for i in range(HALF):
        out[i] = values[i]


def load_kernel(place, tiles, inv, rhs, out, kept_left, kept_right, stage, *scratch):
    left, right, diag, sems, dsems, lsems, rsems = scratch
    leaf = Leaf(left, right, diag)
    kept = (kept_left, kept_right)
    load = Loader(leaf, place, tiles, inv, kept, stage, sems, dsems, lsems, rsems)
    put(out, forward(leaf, [rhs[i] for i in range(HALF)], load))
    load.finish()


def both_kernel(place, kept_left, kept_right, inv, rhs, out, left, right, diag, *sems):
    leaf = Leaf(left, right, diag)
    load = Reloader(leaf, place, inv, (kept_left, kept_right), *sems, range(HALF))
    put(out, backward(leaf, forward(leaf, [rhs[i] for i in range(HALF)], load)))


def backward_kernel(place, kept_left, kept_right, inv, rhs, out, left, right, diag, *sems):
    leaf = Leaf(left, right, diag)
    load = Reloader(leaf, place, inv, (kept_left, kept_right), *sems, range(HALF)[::-1])
    put(out, backward(leaf, [rhs[i] for i in range(HALF)], load))


IN_SMEM = pl.BlockSpec(memory_space=pltpu.SMEM)
IN_VMEM = pl.BlockSpec(memory_space=pltpu.VMEM)
IN_HBM = pl.BlockSpec(memory_space=pltpu.HBM)


def limit(mib):
    return pltpu.CompilerParams(vmem_limit_bytes=mib * 1024 * 1024)


def in_hbm(v):
    return pltpu.with_memory_space_constraint(v, pltpu.HBM)


def leaf_scratch(rank, tile):
    return [
        pltpu.VMEM((TILES, rank, tile), BF),
        pltpu.VMEM((TILES, rank, tile), BF),
        pltpu.VMEM((HALF, tile, tile), BF),
    ]


def leaf_sems():
    dma = pltpu.SemaphoreType.DMA
    return [dma((HALF,)), dma((HALF,)), dma((TILES,))]


def load_and_forward(place, tiles, inv, rhs):
    rank, tile = tiles.shape[1] // 2, tiles.shape[2]
    factors = pltpu.HBM((TILES, rank, tile), BF)
    return pl.pallas_call(
        load_kernel,
        out_shape=(jax.ShapeDtypeStruct(rhs.shape, F32), factors, factors),
        in_specs=[IN_SMEM, IN_HBM, IN_HBM, IN_VMEM],
        out_specs=(IN_VMEM, IN_HBM, IN_HBM),
        scratch_shapes=[
            pltpu.VMEM((SLOTS, HALF - 1, 2 * rank, tile), F32),
            *leaf_scratch(rank, tile),
            pltpu.SemaphoreType.DMA((TILES,)),
            *leaf_sems(),
        ],
        compiler_params=limit(36),
    )(place, in_hbm(tiles), in_hbm(inv), rhs)


def solve(body, place, left, right, inv, rhs):
    return pl.pallas_call(
        body,
        out_shape=jax.ShapeDtypeStruct(rhs.shape, F32),
        in_specs=[IN_SMEM, IN_HBM, IN_HBM, IN_HBM, IN_VMEM],
        out_specs=IN_VMEM,
        scratch_shapes=[*leaf_scratch(*left.shape[1:]), *leaf_sems()],
        compiler_params=limit(24),
    )(place, in_hbm(left), in_hbm(right), in_hbm(inv), rhs)


def per_device(
    root_rhs, diag_inv, tile_u, tile_v, tile_rank, child_x, border_t, child_inv, child_blocks
):
    my_row = lax.axis_index(ROW)
    my_col = lax.axis_index(COL)
    ntile = diag_inv.shape[0]
    tile = diag_inv.shape[1]
    rhs_count = root_rhs.shape[0]
    rank_max = tile_u.shape[4]
    n_child = child_x.shape[0]
    nblk = ntile * tile // BLK
    ndev = lax.axis_size(ALL)
    upper = my_row >= HALF
    in_half = my_row % HALF
    half = lax.axis_index("yh")

    left = tile_u[0, 0, 0]
    live = jnp.arange(rank_max)[None, None, :] < tile_rank[0, 0, 0][:, None, None]
    right = jnp.where(live, tile_v[0, 0, 0].astype(F32), 0.0)

    leaf_u = jnp.where(upper, left[1], left[0]).astype(F32)
    leaf_vt = jnp.where(upper, right[1], right[0]).T
    own_tile = with_layout_constraint(jnp.concatenate([leaf_u, leaf_vt], axis=0), ROWS)
    other_tile = lax.ppermute(own_tile, ALL, plane_pairs())
    upward = jnp.einsum("crs,csb->crb", child_x, border_t, preferred_element_type=F32)
    pieces = (
        upward.reshape(n_child, rhs_count, BB, BLK)
        .transpose(1, 0, 2, 3)
        .reshape(rhs_count, n_child * BB, BLK)
    )
    flat_blocks = child_blocks.reshape(-1)
    dense = jnp.zeros((rhs_count, nblk, BLK), F32).at[:, flat_blocks, :].add(pieces)
    width = ntile * tile // ndev
    parts = dense.reshape(rhs_count, ndev, width).transpose(1, 0, 2)
    mine = lax.all_to_all(parts, ALL, split_axis=0, concat_axis=0, tiled=True)
    mine = mine.sum(axis=0)
    share = jnp.where(my_col < in_half, own_tile, other_tile)
    share = with_layout_constraint(share, ROWS)
    tiles = lax.all_gather(share, PLANE)
    place = jnp.stack([lax.axis_index("yl"), half]).astype(jnp.int32)
    child_sum = copies(mine, HALF_ALL).reshape(ndev // 2, rhs_count, width)
    child_sum = child_sum.transpose(1, 0, 2).reshape(rhs_count, HALF, tile).transpose(1, 0, 2)
    given = root_rhs.reshape(rhs_count, ntile, tile)
    given = lax.dynamic_slice_in_dim(given, HALF * half, HALF, 1)
    own_rhs = given.transpose(1, 0, 2).astype(F32) - child_sum

    x_low, kept_left, kept_right = load_and_forward(place, tiles, diag_inv, own_rhs)
    v0 = right[0].astype(BF)
    u0 = left[0]
    x_col = lax.dynamic_index_in_dim(x_low, my_col, 0, keepdims=False)
    x_own = lax.ppermute(x_col, "yh", [(0, 1)])
    x_own = x_own + jnp.where(upper, 0.0, x_col)
    p = dot_nn(x_own.astype(BF), v0).astype(BF)
    row_sum = copies(dot_nn(p, u0), COL).reshape(8, rhs_count, tile).sum(axis=0)
    row_sums = copies(row_sum, HALF_ROW).reshape(HALF, rhs_count, tile)
    z_high = solve(both_kernel, place, kept_left, kept_right, diag_inv, own_rhs - row_sums)

    z_own = lax.dynamic_index_in_dim(z_high, in_half, 0, keepdims=False).astype(BF)
    q = dot_nt(z_own, u0).astype(BF)
    col_sum = copies(dot_nt(q, v0), ROW).reshape(2, HALF, rhs_count, tile)[1].sum(axis=0)
    col_sums = copies(col_sum, COL).reshape(8, rhs_count, tile)
    low_rhs = x_low - col_sums
    z_low = solve(backward_kernel, place, kept_left, kept_right, diag_inv, low_rhs)
    z_mine = jnp.where(upper, z_high, z_low)
    z_other = lax.ppermute(z_mine, "yh", [(0, 1), (1, 0)])
    low_part = jnp.where(upper, z_other, z_mine)
    high_part = jnp.where(upper, z_mine, z_other)
    result = jnp.concatenate([low_part, high_part], axis=0).transpose(1, 0, 2)
    result = result.reshape(rhs_count, ntile * tile)

    start = (my_row * 8 + my_col) * width
    root_part = lax.dynamic_slice_in_dim(result, start, width, 1)
    gathered = result.reshape(rhs_count, nblk, BLK)[:, flat_blocks, :]
    gathered = gathered.reshape(rhs_count, n_child, BB * BLK).astype(BF)
    returned = jnp.einsum("rcb,csb->crs", gathered, border_t, preferred_element_type=F32)
    child_out = child_x.astype(F32) - jnp.einsum(
        "crs,cst->crt", returned, child_inv.astype(F32)
    )
    return (root_part, child_out)


def solution(mesh):
    finer = Mesh(mesh.devices.reshape(2, 2, 4, 4, 2), ALL)
    in_specs = (
        P(),
        P(),
        P(ROW, COL, None, None, None, None),
        P(ROW, COL, None, None, None, None),
        P(ROW, COL, None, None),
        P(ALL, None, None),
        P(ALL, None, None),
        P(ALL, None, None),
        P(ALL, None),
    )
    out_specs = (P(None, ALL), P(ALL, None, None))
    return jax.shard_map(
        per_device, mesh=finer, in_specs=in_specs, out_specs=out_specs, check_vma=False
    )
```

```python
import functools

import jax
import jax.numpy as jnp
from jax import lax
from jax.experimental import pallas as pl
from jax.experimental.layout import Layout, with_layout_constraint
from jax.experimental.pallas import tpu as pltpu
from jax.sharding import Mesh
from jax.sharding import PartitionSpec as P

BLK = 128
BB = 8
ROW = ("yh", "yl", "z")
HALF_ROW = ("yl", "z")
COL = ("x", "c")
PLANE = ("z", "x", "c")
ALL = ("yh", "yl", "z", "x", "c")
HALF_ALL = ("yl", "z", "x", "c")
HALF = 8
BF = jnp.bfloat16
F32 = jnp.float32
ROWS = Layout((0, 1))


def copies(v, axis):
    n = lax.axis_size(axis)
    stacked = jnp.broadcast_to(v, (n, *v.shape))
    return lax.all_to_all(stacked, axis, split_axis=0, concat_axis=0, tiled=True)


def dot_nn(a, b):
    return lax.dot_general(a, b, (((1,), (0,)), ((), ())), preferred_element_type=F32)


def dot_nt(a, b):
    return lax.dot_general(a, b, (((1,), (1,)), ((), ())), preferred_element_type=F32)


def exact(dot, a, b):
    high = a.astype(BF)
    low = (a - high.astype(F32)).astype(BF)
    both = dot(jnp.concatenate([high, low], axis=0), b)
    n = a.shape[0]
    return both[:n] + both[n:]


def first_tile(row):
    return row * (row - 1) // 2


SLOTS = 3
TILES = first_tile(HALF)
SPARE = {(1, 0): (1, 7), (2, 0): (2, 6), (2, 1): (2, 7), (3, 0): (0, 6), (3, 1): (3, 7), (3, 2): (0, 7)}


def spot(plane, i, k):
    z = i % 4
    own = i // 4 == plane
    if own or (plane == 0 and k >= z):
        return 8 * z + k
    z, k = SPARE[z, k]
    return 8 * z + k


def plane_pairs():
    pairs = []
    for half in range(2):
        for i in range(HALF):
            for k in range(i):
                plane = i // 4
                source = 64 * half + 32 * plane + spot(plane, i, k)
                target = 64 * half + 32 * (1 - plane) + spot(1 - plane, i, k)
                pairs.append((source, target))
    return pairs


class Leaf:
    def __init__(self, left, right, diag):
        self.left, self.right, self.diag = left, right, diag

    def column(self, j):
        return sum(HALF - 1 - m for m in range(j))

    def u(self, i, k, count=1):
        at = first_tile(i) + k
        return self.left[at : at + count].reshape(-1, self.left.shape[2])

    def vt(self, i, k, count=1):
        at = self.column(k) + i - k - 1
        return self.right[at : at + count].reshape(-1, self.right.shape[2])


class Moves:
    def __init__(self, rows):
        self.rows = rows

    def start(self, i):
        for move in self.rows.get(i, []):
            move.start()

    def wait(self, i):
        for move in self.rows.get(i, []):
            move.wait()


def inverse_moves(leaf, first, inv, sems):
    return Moves(
        {
            n: [pltpu.make_async_copy(inv.at[first + n], leaf.diag.at[n], sems.at[n])]
            for n in range(HALF)
        }
    )


def factor_moves(leaf, kept_left, kept_right, lsems, rsems, keep):
    rows = {}
    for i in range(1, HALF):
        at = first_tile(i)
        pairs = [(kept_left.at[pl.ds(at, i)], leaf.left.at[pl.ds(at, i)], lsems.at[i])]
        for k in range(i):
            place = leaf.column(k) + i - k - 1
            pairs.append((kept_right.at[place], leaf.right.at[place], rsems.at[place]))
        rows[i] = [
            pltpu.make_async_copy(*((b, a) if keep else (a, b)), sem) for a, b, sem in pairs
        ]
    return Moves(rows)


class Loader:
    def __init__(self, leaf, place, tiles, inv, kept, stage, sems, dsems, lsems, rsems):
        self.leaf, self.stage = leaf, stage
        rows = {}
        for i in range(1, HALF):
            rows[i] = []
            for k in range(i):
                one, two = spot(0, i, k), spot(1, i, k)
                rows[i].append(
                    pltpu.make_async_copy(
                        tiles.at[one + place[0] * (two - one)],
                        stage.at[i % SLOTS, k],
                        sems.at[first_tile(i) + k],
                    )
                )
        self.tiles = Moves(rows)
        self.inverse = inverse_moves(leaf, HALF * place[1], inv, dsems)
        self.kept = factor_moves(leaf, *kept, lsems, rsems, True)
        for i in range(SLOTS):
            self.start(i)
        self(0)

    def start(self, i):
        self.inverse.start(i)
        self.tiles.start(i)

    def __call__(self, i):
        leaf = self.leaf
        rank = leaf.left.shape[1]
        self.inverse.wait(i)
        self.tiles.wait(i)
        for k in range(i):
            leaf.left[first_tile(i) + k] = self.stage[i % SLOTS, k, :rank].astype(BF)
            leaf.right[leaf.column(k) + i - k - 1] = self.stage[i % SLOTS, k, rank:].astype(BF)
        self.kept.start(i - 1)
        if i + SLOTS < HALF:
            self.start(i + SLOTS)

    def finish(self):
        self.kept.start(HALF - 1)
        for i in range(HALF):
            self.kept.wait(i)


class Reloader:
    def __init__(self, leaf, place, inv, kept, dsems, lsems, rsems, order):
        self.inverse = inverse_moves(leaf, HALF * place[1], inv, dsems)
        self.factors = factor_moves(leaf, *kept, lsems, rsems, False)
        for i in order:
            self.inverse.start(i)
            self.factors.start(i)
        self(order[0])

    def __call__(self, i):
        self.inverse.wait(i)
        self.factors.wait(i)


def forward(leaf, rhs, load=None):
    solved, narrow = [], []
    partial = rhs[0]
    last = None
    for i in range(HALF):
        acc = partial
        if i:
            acc = acc - dot_nn(last, leaf.u(i, i - 1))
        x = exact(dot_nn, acc, leaf.diag[i])
        if i + 1 < HALF:
            if load:
                load(i + 1)
            partial = rhs[i + 1]
            if i:
                known = [dot_nt(narrow[k], leaf.vt(i + 1, k)).astype(BF) for k in range(i)]
                partial = partial - dot_nn(jnp.concatenate(known, axis=1), leaf.u(i + 1, 0, i))
        solved.append(x)
        narrow.append(x.astype(BF))
        if i + 1 < HALF:
            last = dot_nt(narrow[i], leaf.vt(i + 1, i)).astype(BF)
    return solved


def backward(leaf, rhs, load=None):
    width = leaf.left.shape[1]
    solved = [None] * HALF
    waiting = {j: [] for j in range(HALF)}
    partial = rhs[HALF - 1]
    last = None
    for j in reversed(range(HALF)):
        acc = partial
        if j + 1 < HALF:
            acc = acc - dot_nn(last, leaf.vt(j + 1, j))
        z = exact(dot_nt, acc, leaf.diag[j])
        if j:
            if load:
                load(j - 1)
            partial = rhs[j - 1]
            if waiting[j - 1]:
                known = jnp.concatenate(waiting[j - 1][::-1], axis=1)
                partial = partial - dot_nn(known, leaf.vt(j + 1, j - 1, HALF - 1 - j))
        solved[j] = z
        narrow = z.astype(BF)
        if j:
            last = dot_nt(narrow, leaf.u(j, j - 1)).astype(BF)
        if j > 1:
            others = dot_nt(narrow, leaf.u(j, 0, j - 1)).astype(BF)
            for k in range(j - 1):
                waiting[k].append(others[:, k * width : (k + 1) * width])
    return solved


def put(out, values):
    for i in range(HALF):
        out[i] = values[i]


def load_kernel(place, tiles, inv, rhs, out, kept_left, kept_right, stage, *scratch):
    left, right, diag, sems, dsems, lsems, rsems = scratch
    leaf = Leaf(left, right, diag)
    kept = (kept_left, kept_right)
    load = Loader(leaf, place, tiles, inv, kept, stage, sems, dsems, lsems, rsems)
    put(out, forward(leaf, [rhs[i] for i in range(HALF)], load))
    load.finish()


def both_kernel(place, kept_left, kept_right, inv, rhs, out, left, right, diag, *sems):
    leaf = Leaf(left, right, diag)
    load = Reloader(leaf, place, inv, (kept_left, kept_right), *sems, range(HALF))
    put(out, backward(leaf, forward(leaf, [rhs[i] for i in range(HALF)], load)))


def backward_kernel(place, kept_left, kept_right, inv, rhs, out, left, right, diag, *sems):
    leaf = Leaf(left, right, diag)
    load = Reloader(leaf, place, inv, (kept_left, kept_right), *sems, range(HALF)[::-1])
    put(out, backward(leaf, [rhs[i] for i in range(HALF)], load))


IN_SMEM = pl.BlockSpec(memory_space=pltpu.SMEM)
IN_VMEM = pl.BlockSpec(memory_space=pltpu.VMEM)
IN_HBM = pl.BlockSpec(memory_space=pltpu.HBM)


def limit(mib):
    return pltpu.CompilerParams(vmem_limit_bytes=mib * 1024 * 1024)


def in_hbm(v):
    return pltpu.with_memory_space_constraint(v, pltpu.HBM)


def leaf_scratch(rank, tile):
    return [
        pltpu.VMEM((TILES, rank, tile), BF),
        pltpu.VMEM((TILES, rank, tile), BF),
        pltpu.VMEM((HALF, tile, tile), BF),
    ]


def leaf_sems():
    dma = pltpu.SemaphoreType.DMA
    return [dma((HALF,)), dma((HALF,)), dma((TILES,))]


def load_and_forward(place, tiles, inv, rhs):
    rank, tile = tiles.shape[1] // 2, tiles.shape[2]
    factors = pltpu.HBM((TILES, rank, tile), BF)
    return pl.pallas_call(
        load_kernel,
        out_shape=(jax.ShapeDtypeStruct(rhs.shape, F32), factors, factors),
        in_specs=[IN_SMEM, IN_HBM, IN_HBM, IN_VMEM],
        out_specs=(IN_VMEM, IN_HBM, IN_HBM),
        scratch_shapes=[
            pltpu.VMEM((SLOTS, HALF - 1, 2 * rank, tile), F32),
            *leaf_scratch(rank, tile),
            pltpu.SemaphoreType.DMA((TILES,)),
            *leaf_sems(),
        ],
        compiler_params=limit(36),
    )(place, in_hbm(tiles), in_hbm(inv), rhs)


def solve(body, place, left, right, inv, rhs):
    return pl.pallas_call(
        body,
        out_shape=jax.ShapeDtypeStruct(rhs.shape, F32),
        in_specs=[IN_SMEM, IN_HBM, IN_HBM, IN_HBM, IN_VMEM],
        out_specs=IN_VMEM,
        scratch_shapes=[*leaf_scratch(*left.shape[1:]), *leaf_sems()],
        compiler_params=limit(24),
    )(place, in_hbm(left), in_hbm(right), in_hbm(inv), rhs)


def per_device(
    root_rhs, diag_inv, tile_u, tile_v, tile_rank, child_x, border_t, child_inv, child_blocks
):
    my_row = lax.axis_index(ROW)
    my_col = lax.axis_index(COL)
    ntile = diag_inv.shape[0]
    tile = diag_inv.shape[1]
    rhs_count = root_rhs.shape[0]
    rank_max = tile_u.shape[4]
    n_child = child_x.shape[0]
    nblk = ntile * tile // BLK
    ndev = lax.axis_size(ALL)
    upper = my_row >= HALF
    in_half = my_row % HALF
    half = lax.axis_index("yh")

    left = tile_u[0, 0, 0]
    live = jnp.arange(rank_max)[None, None, :] < tile_rank[0, 0, 0][:, None, None]
    right = jnp.where(live, tile_v[0, 0, 0].astype(F32), 0.0)

    leaf_u = jnp.where(upper, left[1], left[0]).astype(F32)
    leaf_vt = jnp.where(upper, right[1], right[0]).T
    own_tile = with_layout_constraint(jnp.concatenate([leaf_u, leaf_vt], axis=0), ROWS)
    other_tile = lax.ppermute(own_tile, ALL, plane_pairs())
    upward = jnp.einsum("crs,csb->crb", child_x, border_t, preferred_element_type=F32)
    pieces = (
        upward.reshape(n_child, rhs_count, BB, BLK)
        .transpose(1, 0, 2, 3)
        .reshape(rhs_count, n_child * BB, BLK)
    )
    flat_blocks = child_blocks.reshape(-1)
    dense = jnp.zeros((rhs_count, nblk, BLK), F32).at[:, flat_blocks, :].add(pieces)
    width = ntile * tile // ndev
    parts = dense.reshape(rhs_count, 4, ntile * tile // 4).transpose(1, 0, 2)
    mine = lax.all_to_all(parts, ("yh", "yl"), split_axis=0, concat_axis=0, tiled=True)
    mine = mine.sum(axis=0).reshape(rhs_count, ndev // 4, width).transpose(1, 0, 2)
    mine = lax.all_to_all(mine, PLANE, split_axis=0, concat_axis=0, tiled=True).sum(axis=0)
    share = jnp.where(my_col < in_half, own_tile, other_tile)
    share = with_layout_constraint(share, ROWS)
    tiles = lax.all_gather(share, PLANE)
    place = jnp.stack([lax.axis_index("yl"), half]).astype(jnp.int32)
    child_sum = copies(mine, HALF_ALL).reshape(ndev // 2, rhs_count, width)
    child_sum = child_sum.transpose(1, 0, 2).reshape(rhs_count, HALF, tile).transpose(1, 0, 2)
    given = root_rhs.reshape(rhs_count, ntile, tile)
    given = lax.dynamic_slice_in_dim(given, HALF * half, HALF, 1)
    own_rhs = given.transpose(1, 0, 2).astype(F32) - child_sum

    x_low, kept_left, kept_right = load_and_forward(place, tiles, diag_inv, own_rhs)
    v0 = right[0].astype(BF)
    u0 = left[0]
    x_col = lax.dynamic_index_in_dim(x_low, my_col, 0, keepdims=False)
    x_own = lax.ppermute(x_col, "yh", [(0, 1)])
    x_own = x_own + jnp.where(upper, 0.0, x_col)
    p = dot_nn(x_own.astype(BF), v0).astype(BF)
    row_sum = copies(dot_nn(p, u0), COL).reshape(8, rhs_count, tile).sum(axis=0)
    row_sums = copies(row_sum, HALF_ROW).reshape(HALF, rhs_count, tile)
    z_high = solve(both_kernel, place, kept_left, kept_right, diag_inv, own_rhs - row_sums)

    z_own = lax.dynamic_index_in_dim(z_high, in_half, 0, keepdims=False).astype(BF)
    q = dot_nt(z_own, u0).astype(BF)
    col_sum = copies(dot_nt(q, v0), ROW).reshape(2, HALF, rhs_count, tile)[1].sum(axis=0)
    col_sums = copies(col_sum, COL).reshape(8, rhs_count, tile)
    low_rhs = x_low - col_sums
    z_low = solve(backward_kernel, place, kept_left, kept_right, diag_inv, low_rhs)
    z_mine = jnp.where(upper, z_high, z_low)
    z_other = lax.ppermute(z_mine, "yh", [(0, 1), (1, 0)])
    low_part = jnp.where(upper, z_other, z_mine)
    high_part = jnp.where(upper, z_mine, z_other)
    result = jnp.concatenate([low_part, high_part], axis=0).transpose(1, 0, 2)
    result = result.reshape(rhs_count, ntile * tile)

    start = (my_row * 8 + my_col) * width
    root_part = lax.dynamic_slice_in_dim(result, start, width, 1)
    gathered = result.reshape(rhs_count, nblk, BLK)[:, flat_blocks, :]
    gathered = gathered.reshape(rhs_count, n_child, BB * BLK).astype(BF)
    returned = jnp.einsum("rcb,csb->crs", gathered, border_t, preferred_element_type=F32)
    child_out = child_x.astype(F32) - jnp.einsum(
        "crs,cst->crt", returned, child_inv.astype(F32)
    )
    return (root_part, child_out)


def solution(mesh):
    finer = Mesh(mesh.devices.reshape(2, 2, 4, 4, 2), ALL)
    in_specs = (
        P(),
        P(),
        P(ROW, COL, None, None, None, None),
        P(ROW, COL, None, None, None, None),
        P(ROW, COL, None, None),
        P(ALL, None, None),
        P(ALL, None, None),
        P(ALL, None, None),
        P(ALL, None),
    )
    out_specs = (P(None, ALL), P(ALL, None, None))
    return jax.shard_map(
        per_device, mesh=finer, in_specs=in_specs, out_specs=out_specs, check_vma=False
    )
```

```python
import functools

import jax
import jax.numpy as jnp
from jax import lax
from jax.experimental import pallas as pl
from jax.experimental.layout import Layout, with_layout_constraint
from jax.experimental.pallas import tpu as pltpu
from jax.sharding import Mesh
from jax.sharding import PartitionSpec as P

BLK = 128
BB = 8
ROW = ("yh", "yl", "z")
HALF_ROW = ("yl", "z")
COL = ("x", "c")
PLANE = ("z", "x", "c")
ALL = ("yh", "yl", "z", "x", "c")
HALF_ALL = ("yl", "z", "x", "c")
HALF = 8
BF = jnp.bfloat16
F32 = jnp.float32
ROWS = Layout((0, 1))


def copies(v, axis):
    n = lax.axis_size(axis)
    stacked = jnp.broadcast_to(v, (n, *v.shape))
    return lax.all_to_all(stacked, axis, split_axis=0, concat_axis=0, tiled=True)


def dot_nn(a, b):
    return lax.dot_general(a, b, (((1,), (0,)), ((), ())), preferred_element_type=F32)


def dot_nt(a, b):
    return lax.dot_general(a, b, (((1,), (1,)), ((), ())), preferred_element_type=F32)


def exact(dot, a, b):
    high = a.astype(BF)
    low = (a - high.astype(F32)).astype(BF)
    both = dot(jnp.concatenate([high, low], axis=0), b)
    n = a.shape[0]
    return both[:n] + both[n:]


def first_tile(row):
    return row * (row - 1) // 2


SLOTS = 3
TILES = first_tile(HALF)
SPARE = {(1, 0): (1, 7), (2, 0): (2, 6), (2, 1): (2, 7), (3, 0): (0, 6), (3, 1): (3, 7), (3, 2): (0, 7)}


def spot(plane, i, k):
    z = i % 4
    own = i // 4 == plane
    if own or (plane == 0 and k >= z):
        return 8 * z + k
    z, k = SPARE[z, k]
    return 8 * z + k


def plane_pairs():
    pairs = []
    for half in range(2):
        for i in range(HALF):
            for k in range(i):
                plane = i // 4
                source = 64 * half + 32 * plane + spot(plane, i, k)
                target = 64 * half + 32 * (1 - plane) + spot(1 - plane, i, k)
                pairs.append((source, target))
    return pairs


class Leaf:
    def __init__(self, left, right, diag=None, flipped=None):
        self.left, self.right, self.diag, self.flipped = left, right, diag, flipped

    def column(self, j):
        return sum(HALF - 1 - m for m in range(j))

    def u(self, i, k, count=1):
        at = first_tile(i) + k
        return self.left[at : at + count].reshape(-1, self.left.shape[2])

    def vt(self, i, k, count=1):
        at = self.column(k) + i - k - 1
        return self.right[at : at + count].reshape(-1, self.right.shape[2])


class Moves:
    def __init__(self, rows):
        self.rows = rows

    def start(self, i):
        for move in self.rows.get(i, []):
            move.start()

    def wait(self, i):
        for move in self.rows.get(i, []):
            move.wait()


def inverse_moves(target, first, source, sems):
    return Moves(
        {
            n: [pltpu.make_async_copy(source.at[first + n], target.at[n], sems.at[n])]
            for n in range(HALF)
        }
    )


def factor_moves(leaf, kept_left, kept_right, lsems, rsems, keep):
    rows = {}
    for i in range(1, HALF):
        at = first_tile(i)
        pairs = [(kept_left.at[pl.ds(at, i)], leaf.left.at[pl.ds(at, i)], lsems.at[i])]
        for k in range(i):
            place = leaf.column(k) + i - k - 1
            pairs.append((kept_right.at[place], leaf.right.at[place], rsems.at[place]))
        rows[i] = [
            pltpu.make_async_copy(*((b, a) if keep else (a, b)), sem) for a, b, sem in pairs
        ]
    return Moves(rows)


class Loader:
    def __init__(self, leaf, place, tiles, stage, sems, kept=None, inverse=None):
        self.leaf, self.stage = leaf, stage
        rows = {}
        for i in range(1, HALF):
            rows[i] = []
            for k in range(i):
                one, two = spot(0, i, k), spot(1, i, k)
                rows[i].append(
                    pltpu.make_async_copy(
                        tiles.at[one + place[0] * (two - one)],
                        stage.at[i % SLOTS, k],
                        sems.at[first_tile(i) + k],
                    )
                )
        self.tiles = Moves(rows)
        self.inverse = inverse or Moves({})
        self.kept = kept or Moves({})
        for i in range(SLOTS):
            self.start(i)
        self(0)

    def start(self, i):
        self.inverse.start(i)
        self.tiles.start(i)

    def __call__(self, i):
        leaf = self.leaf
        rank = leaf.left.shape[1]
        self.inverse.wait(i)
        self.tiles.wait(i)
        for k in range(i):
            leaf.left[first_tile(i) + k] = self.stage[i % SLOTS, k, :rank].astype(BF)
            leaf.right[leaf.column(k) + i - k - 1] = self.stage[i % SLOTS, k, rank:].astype(BF)
        self.kept.start(i - 1)
        if i + SLOTS < HALF:
            self.start(i + SLOTS)


class Reloader:
    def __init__(self, inverse, factors, order):
        self.inverse, self.factors = inverse, factors
        for i in order:
            inverse.start(i)
            factors.start(i)
        self(order[0])

    def __call__(self, i):
        self.inverse.wait(i)
        self.factors.wait(i)


def forward(leaf, rhs, load=None):
    solved, narrow = [], []
    partial = rhs[0]
    last = None
    for i in range(HALF):
        acc = partial
        if i:
            acc = acc - dot_nn(last, leaf.u(i, i - 1))
        x = exact(dot_nn, acc, leaf.diag[i])
        if i + 1 < HALF:
            if load:
                load(i + 1)
            partial = rhs[i + 1]
            if i:
                known = [dot_nt(narrow[k], leaf.vt(i + 1, k)).astype(BF) for k in range(i)]
                partial = partial - dot_nn(jnp.concatenate(known, axis=1), leaf.u(i + 1, 0, i))
        solved.append(x)
        narrow.append(x.astype(BF))
        if i + 1 < HALF:
            last = dot_nt(narrow[i], leaf.vt(i + 1, i)).astype(BF)
    return solved


def backward(leaf, rhs, load=None):
    width = leaf.left.shape[1]
    solved = [None] * HALF
    waiting = {j: [] for j in range(HALF)}
    partial = rhs[HALF - 1]
    last = None
    for j in reversed(range(HALF)):
        acc = partial
        if j + 1 < HALF:
            acc = acc - dot_nn(last, leaf.vt(j + 1, j))
        z = exact(dot_nn, acc, leaf.flipped[j])
        if j:
            if load:
                load(j - 1)
            partial = rhs[j - 1]
            if waiting[j - 1]:
                known = jnp.concatenate(waiting[j - 1][::-1], axis=1)
                partial = partial - dot_nn(known, leaf.vt(j + 1, j - 1, HALF - 1 - j))
        solved[j] = z
        narrow = z.astype(BF)
        if j:
            last = dot_nt(narrow, leaf.u(j, j - 1)).astype(BF)
        if j > 1:
            others = dot_nt(narrow, leaf.u(j, 0, j - 1)).astype(BF)
            for k in range(j - 1):
                waiting[k].append(others[:, k * width : (k + 1) * width])
    return solved


def put(out, values):
    for i in range(HALF):
        out[i] = values[i]


def values(ref):
    return [ref[i] for i in range(HALF)]


def keep_tiles(leaf, place, tiles, stage, sems, kept, lsems, rsems):
    moves = factor_moves(leaf, *kept, lsems, rsems, True)
    load = Loader(leaf, place, tiles, stage, sems, kept=moves)
    for i in range(1, HALF):
        load(i)
    moves.start(HALF - 1)
    for i in range(HALF):
        moves.wait(i)


def first_kernel(place, tiles, inv, rhs, out, kept_left, kept_right, stage, *scratch):
    left, right, diag, sems, dsems, lsems, rsems = scratch
    leaf = Leaf(left, right, diag)

    @pl.when(place[1] == 0)
    def _():
        inverse = inverse_moves(diag, 0, inv, dsems)
        load = Loader(leaf, place, tiles, stage, sems, inverse=inverse)
        put(out, forward(leaf, values(rhs), load))

    @pl.when(place[1] == 1)
    def _():
        out[...] = jnp.zeros(out.shape, F32)
        keep_tiles(leaf, place, tiles, stage, sems, (kept_left, kept_right), lsems, rsems)


def second_kernel(place, tiles, kept_left, kept_right, inv, turned, rhs, *refs):
    out, next_left, next_right, stage, left, right, diag, flipped = refs[:8]
    sems, dsems, tsems, lsems, rsems = refs[8:]
    leaf = Leaf(left, right, diag, flipped)

    @pl.when(place[1] == 0)
    def _():
        out[...] = jnp.zeros(out.shape, F32)
        keep_tiles(leaf, place, tiles, stage, sems, (next_left, next_right), lsems, rsems)

    @pl.when(place[1] == 1)
    def _():
        inverse = inverse_moves(diag, HALF, inv, dsems)
        factors = factor_moves(leaf, kept_left, kept_right, lsems, rsems, False)
        load = Reloader(inverse, factors, range(HALF))
        turn = inverse_moves(flipped, 0, turned, tsems)
        for n in range(HALF):
            turn.start(n)
        solved = forward(leaf, values(rhs), load)
        for n in range(HALF):
            turn.wait(n)
        put(out, backward(leaf, solved))


def third_kernel(place, kept_left, kept_right, turned, rhs, out, left, right, flipped, *sems):
    tsems, lsems, rsems = sems
    leaf = Leaf(left, right, flipped=flipped)

    @pl.when(place[1] == 0)
    def _():
        turn = inverse_moves(flipped, 0, turned, tsems)
        factors = factor_moves(leaf, kept_left, kept_right, lsems, rsems, False)
        load = Reloader(turn, factors, range(HALF)[::-1])
        put(out, backward(leaf, values(rhs), load))

    @pl.when(place[1] == 1)
    def _():
        out[...] = jnp.zeros(out.shape, F32)


IN_SMEM = pl.BlockSpec(memory_space=pltpu.SMEM)
IN_VMEM = pl.BlockSpec(memory_space=pltpu.VMEM)
IN_HBM = pl.BlockSpec(memory_space=pltpu.HBM)


def limit(mib):
    return pltpu.CompilerParams(vmem_limit_bytes=mib * 1024 * 1024)


def in_hbm(v):
    return pltpu.with_memory_space_constraint(v, pltpu.HBM)


def solve(body, place, hbm, rhs, keeps, loads, inverses):
    tile = rhs.shape[2]
    rank = tile // 4
    dma = pltpu.SemaphoreType.DMA
    solved = jax.ShapeDtypeStruct(rhs.shape, F32)
    factors = pltpu.HBM((TILES, rank, tile), BF)
    return pl.pallas_call(
        body,
        out_shape=(solved, factors, factors) if keeps else solved,
        in_specs=[IN_SMEM, *[IN_HBM] * len(hbm), IN_VMEM],
        out_specs=(IN_VMEM, IN_HBM, IN_HBM) if keeps else IN_VMEM,
        scratch_shapes=[
            *[pltpu.VMEM((SLOTS, HALF - 1, 2 * rank, tile), F32)] * loads,
            *[pltpu.VMEM((TILES, rank, tile), BF)] * 2,
            *[pltpu.VMEM((HALF, tile, tile), BF)] * inverses,
            *[dma((TILES,))] * loads,
            *[dma((HALF,))] * inverses,
            dma((HALF,)),
            dma((TILES,)),
        ],
        compiler_params=limit(40),
    )(place, *[in_hbm(v) for v in hbm], rhs)


def per_device(
    root_rhs, diag_inv, tile_u, tile_v, tile_rank, child_x, border_t, child_inv, child_blocks
):
    my_row = lax.axis_index(ROW)
    my_col = lax.axis_index(COL)
    ntile = diag_inv.shape[0]
    tile = diag_inv.shape[1]
    rhs_count = root_rhs.shape[0]
    rank_max = tile_u.shape[4]
    n_child = child_x.shape[0]
    nblk = ntile * tile // BLK
    ndev = lax.axis_size(ALL)
    upper = my_row >= HALF
    in_half = my_row % HALF
    half = lax.axis_index("yh")

    left = tile_u[0, 0, 0]
    live = jnp.arange(rank_max)[None, None, :] < tile_rank[0, 0, 0][:, None, None]
    right = jnp.where(live, tile_v[0, 0, 0].astype(F32), 0.0)

    leaf_u = jnp.where(upper, left[1], left[0]).astype(F32)
    leaf_vt = jnp.where(upper, right[1], right[0]).T
    own_tile = with_layout_constraint(jnp.concatenate([leaf_u, leaf_vt], axis=0), ROWS)
    other_tile = lax.ppermute(own_tile, ALL, plane_pairs())
    upward = jnp.einsum("crs,csb->crb", child_x, border_t, preferred_element_type=F32)
    pieces = (
        upward.reshape(n_child, rhs_count, BB, BLK)
        .transpose(1, 0, 2, 3)
        .reshape(rhs_count, n_child * BB, BLK)
    )
    flat_blocks = child_blocks.reshape(-1)
    dense = jnp.zeros((rhs_count, nblk, BLK), F32).at[:, flat_blocks, :].add(pieces)
    width = ntile * tile // ndev
    parts = dense.reshape(rhs_count * 4, ndev // 4, width).transpose(1, 0, 2)
    mine = lax.all_to_all(parts, PLANE, split_axis=0, concat_axis=0, tiled=True).sum(axis=0)
    other_tile, mine = lax.optimization_barrier((other_tile, mine))
    mine = mine.reshape(rhs_count, 4, width).transpose(1, 0, 2)
    mine = lax.all_to_all(mine, ("yh", "yl"), split_axis=0, concat_axis=0, tiled=True)
    mine = mine.sum(axis=0)
    share = jnp.where(my_col < in_half, own_tile, other_tile)
    share = with_layout_constraint(share, ROWS)
    tiles = lax.all_gather(share, PLANE)
    place = jnp.stack([lax.axis_index("yl"), half]).astype(jnp.int32)
    child_sum = copies(mine, HALF_ALL).reshape(ndev // 2, rhs_count, width)
    child_sum = child_sum.transpose(1, 0, 2).reshape(rhs_count, HALF, tile).transpose(1, 0, 2)
    given = root_rhs.reshape(rhs_count, ntile, tile)
    given = lax.dynamic_slice_in_dim(given, HALF * half, HALF, 1)
    own_rhs = given.transpose(1, 0, 2).astype(F32) - child_sum
    begin, own_rhs = lax.optimization_barrier((HALF * half, own_rhs))
    turned = lax.dynamic_slice_in_dim(diag_inv, begin, HALF, 0).transpose(0, 2, 1)

    x_low, *kept = solve(first_kernel, place, [tiles, diag_inv], own_rhs, True, 1, 1)
    v0 = right[0].astype(BF)
    u0 = left[0]
    x_col = lax.dynamic_index_in_dim(x_low, my_col, 0, keepdims=False)
    x_own = lax.ppermute(x_col, "yh", [(0, 1)])
    x_own = x_own + jnp.where(upper, 0.0, x_col)
    p = dot_nn(x_own.astype(BF), v0).astype(BF)
    row_sum = copies(dot_nn(p, u0), COL).reshape(8, rhs_count, tile).sum(axis=0)
    row_sums = copies(row_sum, HALF_ROW).reshape(HALF, rhs_count, tile)
    arrays = [tiles, *kept, diag_inv, turned]
    z_high, *kept = solve(second_kernel, place, arrays, own_rhs - row_sums, True, 1, 2)

    z_own = lax.dynamic_index_in_dim(z_high, in_half, 0, keepdims=False).astype(BF)
    q = dot_nt(z_own, u0).astype(BF)
    col_sum = copies(dot_nt(q, v0), ROW).reshape(2, HALF, rhs_count, tile)[1].sum(axis=0)
    col_sums = copies(col_sum, COL).reshape(8, rhs_count, tile)
    low_rhs = x_low - col_sums
    z_low = solve(third_kernel, place, [*kept, turned], low_rhs, False, 0, 1)
    z_mine = jnp.where(upper, z_high, z_low)
    z_other = lax.ppermute(z_mine, "yh", [(0, 1), (1, 0)])
    low_part = jnp.where(upper, z_other, z_mine)
    high_part = jnp.where(upper, z_mine, z_other)
    result = jnp.concatenate([low_part, high_part], axis=0).transpose(1, 0, 2)
    result = result.reshape(rhs_count, ntile * tile)

    start = (my_row * 8 + my_col) * width
    root_part = lax.dynamic_slice_in_dim(result, start, width, 1)
    gathered = result.reshape(rhs_count, nblk, BLK)[:, flat_blocks, :]
    gathered = gathered.reshape(rhs_count, n_child, BB * BLK).astype(BF)
    returned = jnp.einsum("rcb,csb->crs", gathered, border_t, preferred_element_type=F32)
    child_out = child_x.astype(F32) - jnp.einsum(
        "crs,cst->crt", returned, child_inv.astype(F32)
    )
    return (root_part, child_out)


def solution(mesh):
    finer = Mesh(mesh.devices.reshape(2, 2, 4, 4, 2), ALL)
    in_specs = (
        P(),
        P(),
        P(ROW, COL, None, None, None, None),
        P(ROW, COL, None, None, None, None),
        P(ROW, COL, None, None),
        P(ALL, None, None),
        P(ALL, None, None),
        P(ALL, None, None),
        P(ALL, None),
    )
    out_specs = (P(None, ALL), P(ALL, None, None))
    return jax.shard_map(
        per_device, mesh=finer, in_specs=in_specs, out_specs=out_specs, check_vma=False
    )
```

```python
import functools

import jax
import jax.numpy as jnp
from jax import lax
from jax.experimental import pallas as pl
from jax.experimental.layout import Layout, with_layout_constraint
from jax.experimental.pallas import tpu as pltpu
from jax.sharding import Mesh
from jax.sharding import PartitionSpec as P

BLK = 128
BB = 8
ROW = ("yh", "yl", "z")
HALF_ROW = ("yl", "z")
COL = ("x", "c")
PLANE = ("z", "x", "c")
ALL = ("yh", "yl", "z", "x", "c")
HALF_ALL = ("yl", "z", "x", "c")
HALF = 8
BF = jnp.bfloat16
F32 = jnp.float32
ROWS = Layout((0, 1))


def copies(v, axis):
    n = lax.axis_size(axis)
    stacked = jnp.broadcast_to(v, (n, *v.shape))
    return lax.all_to_all(stacked, axis, split_axis=0, concat_axis=0, tiled=True)


def dot_nn(a, b):
    return lax.dot_general(a, b, (((1,), (0,)), ((), ())), preferred_element_type=F32)


def dot_nt(a, b):
    return lax.dot_general(a, b, (((1,), (1,)), ((), ())), preferred_element_type=F32)


def exact(dot, a, b):
    high = a.astype(BF)
    low = (a - high.astype(F32)).astype(BF)
    both = dot(jnp.concatenate([high, low], axis=0), b)
    n = a.shape[0]
    return both[:n] + both[n:]


def first_tile(row):
    return row * (row - 1) // 2


SLOTS = 3
TILES = first_tile(HALF)
SPARE = {(1, 0): (1, 7), (2, 0): (2, 6), (2, 1): (2, 7), (3, 0): (0, 6), (3, 1): (3, 7), (3, 2): (0, 7)}


def spot(plane, i, k):
    z = i % 4
    own = i // 4 == plane
    if own or (plane == 0 and k >= z):
        return 8 * z + k
    z, k = SPARE[z, k]
    return 8 * z + k


def plane_pairs():
    pairs = []
    for half in range(2):
        for i in range(HALF):
            for k in range(i):
                plane = i // 4
                source = 64 * half + 32 * plane + spot(plane, i, k)
                target = 64 * half + 32 * (1 - plane) + spot(1 - plane, i, k)
                pairs.append((source, target))
    return pairs


class Leaf:
    def __init__(self, left, right, diag):
        self.left, self.right, self.diag = left, right, diag

    def column(self, j):
        return sum(HALF - 1 - m for m in range(j))

    def u(self, i, k, count=1):
        at = first_tile(i) + k
        return self.left[at : at + count].reshape(-1, self.left.shape[2])

    def vt(self, i, k, count=1):
        at = self.column(k) + i - k - 1
        return self.right[at : at + count].reshape(-1, self.right.shape[2])


class Moves:
    def __init__(self, rows):
        self.rows = rows

    def start(self, i):
        for move in self.rows.get(i, []):
            move.start()

    def wait(self, i):
        for move in self.rows.get(i, []):
            move.wait()


def inverse_moves(target, first, source, sems):
    return Moves(
        {
            n: [pltpu.make_async_copy(source.at[first + n], target.at[n], sems.at[n])]
            for n in range(HALF)
        }
    )


def factor_moves(leaf, kept_left, kept_right, lsems, rsems, keep):
    rows = {}
    for i in range(1, HALF):
        at = first_tile(i)
        pairs = [(kept_left.at[pl.ds(at, i)], leaf.left.at[pl.ds(at, i)], lsems.at[i])]
        for k in range(i):
            place = leaf.column(k) + i - k - 1
            pairs.append((kept_right.at[place], leaf.right.at[place], rsems.at[place]))
        rows[i] = [
            pltpu.make_async_copy(*((b, a) if keep else (a, b)), sem) for a, b, sem in pairs
        ]
    return Moves(rows)


class Loader:
    def __init__(self, leaf, place, tiles, stage, sems, kept=None, inverse=None):
        self.leaf, self.stage = leaf, stage
        rows = {}
        for i in range(1, HALF):
            rows[i] = []
            for k in range(i):
                one, two = spot(0, i, k), spot(1, i, k)
                rows[i].append(
                    pltpu.make_async_copy(
                        tiles.at[one + place[0] * (two - one)],
                        stage.at[i % SLOTS, k],
                        sems.at[first_tile(i) + k],
                    )
                )
        self.tiles = Moves(rows)
        self.inverse = inverse or Moves({})
        self.kept = kept or Moves({})
        for i in range(SLOTS):
            self.start(i)
        self(0)

    def start(self, i):
        self.inverse.start(i)
        self.tiles.start(i)

    def __call__(self, i):
        leaf = self.leaf
        rank = leaf.left.shape[1]
        self.inverse.wait(i)
        self.tiles.wait(i)
        for k in range(i):
            leaf.left[first_tile(i) + k] = self.stage[i % SLOTS, k, :rank].astype(BF)
            leaf.right[leaf.column(k) + i - k - 1] = self.stage[i % SLOTS, k, rank:].astype(BF)
        self.kept.start(i - 1)
        if i + SLOTS < HALF:
            self.start(i + SLOTS)


class Reloader:
    def __init__(self, inverse, factors, order):
        self.inverse, self.factors = inverse, factors
        for i in order:
            inverse.start(i)
            factors.start(i)
        self(order[0])

    def __call__(self, i):
        self.inverse.wait(i)
        self.factors.wait(i)


def forward(leaf, rhs, load=None):
    solved, narrow = [], []
    partial = rhs[0]
    last = None
    for i in range(HALF):
        acc = partial
        if i:
            acc = acc - dot_nn(last, leaf.u(i, i - 1))
        x = exact(dot_nn, acc, leaf.diag[i])
        if i + 1 < HALF:
            if load:
                load(i + 1)
            partial = rhs[i + 1]
            if i:
                known = [dot_nt(narrow[k], leaf.vt(i + 1, k)).astype(BF) for k in range(i)]
                partial = partial - dot_nn(jnp.concatenate(known, axis=1), leaf.u(i + 1, 0, i))
        solved.append(x)
        narrow.append(x.astype(BF))
        if i + 1 < HALF:
            last = dot_nt(narrow[i], leaf.vt(i + 1, i)).astype(BF)
    return solved


def backward(leaf, rhs, load=None):
    width = leaf.left.shape[1]
    solved = [None] * HALF
    waiting = {j: [] for j in range(HALF)}
    partial = rhs[HALF - 1]
    last = None
    for j in reversed(range(HALF)):
        acc = partial
        if j + 1 < HALF:
            acc = acc - dot_nn(last, leaf.vt(j + 1, j))
        z = exact(dot_nt, acc, leaf.diag[j])
        if j:
            if load:
                load(j - 1)
            partial = rhs[j - 1]
            if waiting[j - 1]:
                known = jnp.concatenate(waiting[j - 1][::-1], axis=1)
                partial = partial - dot_nn(known, leaf.vt(j + 1, j - 1, HALF - 1 - j))
        solved[j] = z
        narrow = z.astype(BF)
        if j:
            last = dot_nt(narrow, leaf.u(j, j - 1)).astype(BF)
        if j > 1:
            others = dot_nt(narrow, leaf.u(j, 0, j - 1)).astype(BF)
            for k in range(j - 1):
                waiting[k].append(others[:, k * width : (k + 1) * width])
    return solved


def put(out, values):
    for i in range(HALF):
        out[i] = values[i]


def values(ref):
    return [ref[i] for i in range(HALF)]


def keep_tiles(leaf, place, tiles, stage, sems, kept, lsems, rsems):
    moves = factor_moves(leaf, *kept, lsems, rsems, True)
    load = Loader(leaf, place, tiles, stage, sems, kept=moves)
    for i in range(1, HALF):
        load(i)
    moves.start(HALF - 1)
    for i in range(HALF):
        moves.wait(i)


def first_kernel(place, tiles, inv, rhs, out, kept_left, kept_right, stage, *scratch):
    left, right, diag, sems, dsems, lsems, rsems = scratch
    leaf = Leaf(left, right, diag)

    @pl.when(place[1] == 0)
    def _():
        inverse = inverse_moves(diag, 0, inv, dsems)
        load = Loader(leaf, place, tiles, stage, sems, inverse=inverse)
        put(out, forward(leaf, values(rhs), load))

    @pl.when(place[1] == 1)
    def _():
        out[...] = jnp.zeros(out.shape, F32)
        keep_tiles(leaf, place, tiles, stage, sems, (kept_left, kept_right), lsems, rsems)


def second_kernel(place, tiles, kept_left, kept_right, inv, rhs, *refs):
    out, next_left, next_right, stage, left, right, diag, sems, dsems, lsems, rsems = refs
    leaf = Leaf(left, right, diag)

    @pl.when(place[1] == 0)
    def _():
        out[...] = jnp.zeros(out.shape, F32)
        keep_tiles(leaf, place, tiles, stage, sems, (next_left, next_right), lsems, rsems)

    @pl.when(place[1] == 1)
    def _():
        inverse = inverse_moves(diag, HALF, inv, dsems)
        factors = factor_moves(leaf, kept_left, kept_right, lsems, rsems, False)
        load = Reloader(inverse, factors, range(HALF))
        put(out, backward(leaf, forward(leaf, values(rhs), load)))


def third_kernel(place, kept_left, kept_right, inv, rhs, out, left, right, diag, *sems):
    dsems, lsems, rsems = sems
    leaf = Leaf(left, right, diag)

    @pl.when(place[1] == 0)
    def _():
        inverse = inverse_moves(diag, 0, inv, dsems)
        factors = factor_moves(leaf, kept_left, kept_right, lsems, rsems, False)
        load = Reloader(inverse, factors, range(HALF)[::-1])
        put(out, backward(leaf, values(rhs), load))

    @pl.when(place[1] == 1)
    def _():
        out[...] = jnp.zeros(out.shape, F32)


IN_SMEM = pl.BlockSpec(memory_space=pltpu.SMEM)
IN_VMEM = pl.BlockSpec(memory_space=pltpu.VMEM)
IN_HBM = pl.BlockSpec(memory_space=pltpu.HBM)


def limit(mib):
    return pltpu.CompilerParams(vmem_limit_bytes=mib * 1024 * 1024)


def in_hbm(v):
    return pltpu.with_memory_space_constraint(v, pltpu.HBM)


def solve(body, place, hbm, rhs, keeps, loads):
    tile = rhs.shape[2]
    rank = tile // 4
    dma = pltpu.SemaphoreType.DMA
    solved = jax.ShapeDtypeStruct(rhs.shape, F32)
    factors = pltpu.HBM((TILES, rank, tile), BF)
    return pl.pallas_call(
        body,
        out_shape=(solved, factors, factors) if keeps else solved,
        in_specs=[IN_SMEM, *[IN_HBM] * len(hbm), IN_VMEM],
        out_specs=(IN_VMEM, IN_HBM, IN_HBM) if keeps else IN_VMEM,
        scratch_shapes=[
            *[pltpu.VMEM((SLOTS, HALF - 1, 2 * rank, tile), F32)] * loads,
            *[pltpu.VMEM((TILES, rank, tile), BF)] * 2,
            pltpu.VMEM((HALF, tile, tile), BF),
            *[dma((TILES,))] * loads,
            dma((HALF,)),
            dma((HALF,)),
            dma((TILES,)),
        ],
        compiler_params=limit(40),
    )(place, *[in_hbm(v) for v in hbm], rhs)


def per_device(
    root_rhs, diag_inv, tile_u, tile_v, tile_rank, child_x, border_t, child_inv, child_blocks
):
    my_row = lax.axis_index(ROW)
    my_col = lax.axis_index(COL)
    ntile = diag_inv.shape[0]
    tile = diag_inv.shape[1]
    rhs_count = root_rhs.shape[0]
    rank_max = tile_u.shape[4]
    n_child = child_x.shape[0]
    nblk = ntile * tile // BLK
    ndev = lax.axis_size(ALL)
    upper = my_row >= HALF
    in_half = my_row % HALF
    half = lax.axis_index("yh")

    left = tile_u[0, 0, 0]
    live = jnp.arange(rank_max)[None, None, :] < tile_rank[0, 0, 0][:, None, None]
    right = jnp.where(live, tile_v[0, 0, 0].astype(F32), 0.0)

    leaf_u = jnp.where(upper, left[1], left[0]).astype(F32)
    leaf_vt = jnp.where(upper, right[1], right[0]).T
    own_tile = with_layout_constraint(jnp.concatenate([leaf_u, leaf_vt], axis=0), ROWS)
    other_tile = lax.ppermute(own_tile, ALL, plane_pairs())
    upward = jnp.einsum("crs,csb->crb", child_x, border_t, preferred_element_type=F32)
    pieces = (
        upward.reshape(n_child, rhs_count, BB, BLK)
        .transpose(1, 0, 2, 3)
        .reshape(rhs_count, n_child * BB, BLK)
    )
    flat_blocks = child_blocks.reshape(-1)
    dense = jnp.zeros((rhs_count, nblk, BLK), F32).at[:, flat_blocks, :].add(pieces)
    width = ntile * tile // ndev
    parts = dense.reshape(rhs_count, 4, ntile * tile // 4).transpose(1, 0, 2)
    mine = lax.all_to_all(parts, ("yh", "yl"), split_axis=0, concat_axis=0, tiled=True)
    mine = mine.sum(axis=0).reshape(rhs_count, ndev // 4, width).transpose(1, 0, 2)
    mine = lax.all_to_all(mine, PLANE, split_axis=0, concat_axis=0, tiled=True).sum(axis=0)
    share = jnp.where(my_col < in_half, own_tile, other_tile)
    share = with_layout_constraint(share, ROWS)
    tiles = lax.all_gather(share, PLANE)
    place = jnp.stack([lax.axis_index("yl"), half]).astype(jnp.int32)
    child_sum = copies(mine, HALF_ALL).reshape(ndev // 2, rhs_count, width)
    child_sum = child_sum.transpose(1, 0, 2).reshape(rhs_count, HALF, tile).transpose(1, 0, 2)
    given = root_rhs.reshape(rhs_count, ntile, tile)
    given = lax.dynamic_slice_in_dim(given, HALF * half, HALF, 1)
    own_rhs = given.transpose(1, 0, 2).astype(F32) - child_sum

    x_low, *kept = solve(first_kernel, place, [tiles, diag_inv], own_rhs, True, 1)
    v0 = right[0].astype(BF)
    u0 = left[0]
    x_col = lax.dynamic_index_in_dim(x_low, my_col, 0, keepdims=False)
    x_own = lax.ppermute(x_col, "yh", [(0, 1)])
    x_own = x_own + jnp.where(upper, 0.0, x_col)
    p = dot_nn(x_own.astype(BF), v0).astype(BF)
    row_sum = copies(dot_nn(p, u0), COL).reshape(8, rhs_count, tile).sum(axis=0)
    row_sums = copies(row_sum, HALF_ROW).reshape(HALF, rhs_count, tile)
    arrays = [tiles, *kept, diag_inv]
    z_high, *kept = solve(second_kernel, place, arrays, own_rhs - row_sums, True, 1)

    z_own = lax.dynamic_index_in_dim(z_high, in_half, 0, keepdims=False).astype(BF)
    q = dot_nt(z_own, u0).astype(BF)
    col_sum = copies(dot_nt(q, v0), ROW).reshape(2, HALF, rhs_count, tile)[1].sum(axis=0)
    col_sums = copies(col_sum, COL).reshape(8, rhs_count, tile)
    low_rhs = x_low - col_sums
    z_low = solve(third_kernel, place, [*kept, diag_inv], low_rhs, False, 0)
    z_mine = jnp.where(upper, z_high, z_low)
    z_other = lax.ppermute(z_mine, "yh", [(0, 1), (1, 0)])
    low_part = jnp.where(upper, z_other, z_mine)
    high_part = jnp.where(upper, z_mine, z_other)
    result = jnp.concatenate([low_part, high_part], axis=0).transpose(1, 0, 2)
    result = result.reshape(rhs_count, ntile * tile)

    start = (my_row * 8 + my_col) * width
    root_part = lax.dynamic_slice_in_dim(result, start, width, 1)
    gathered = result.reshape(rhs_count, nblk, BLK)[:, flat_blocks, :]
    gathered = gathered.reshape(rhs_count, n_child, BB * BLK).astype(BF)
    returned = jnp.einsum("rcb,csb->crs", gathered, border_t, preferred_element_type=F32)
    child_out = child_x.astype(F32) - jnp.einsum(
        "crs,cst->crt", returned, child_inv.astype(F32)
    )
    return (root_part, child_out)


def solution(mesh):
    finer = Mesh(mesh.devices.reshape(2, 2, 4, 4, 2), ALL)
    in_specs = (
        P(),
        P(),
        P(ROW, COL, None, None, None, None),
        P(ROW, COL, None, None, None, None),
        P(ROW, COL, None, None),
        P(ALL, None, None),
        P(ALL, None, None),
        P(ALL, None, None),
        P(ALL, None),
    )
    out_specs = (P(None, ALL), P(ALL, None, None))
    return jax.shard_map(
        per_device, mesh=finer, in_specs=in_specs, out_specs=out_specs, check_vma=False
    )
```

```python
import functools

import jax
import jax.numpy as jnp
from jax import lax
from jax.experimental import pallas as pl
from jax.experimental.layout import Layout, with_layout_constraint
from jax.experimental.pallas import tpu as pltpu
from jax.sharding import Mesh
from jax.sharding import PartitionSpec as P

BLK = 128
BB = 8
ROW = ("yh", "yl", "z")
HALF_ROW = ("yl", "z")
COL = ("x", "c")
PLANE = ("z", "x", "c")
ALL = ("yh", "yl", "z", "x", "c")
HALF_ALL = ("yl", "z", "x", "c")
HALF = 8
BF = jnp.bfloat16
F32 = jnp.float32
ROWS = Layout((0, 1))


def copies(v, axis):
    n = lax.axis_size(axis)
    stacked = jnp.broadcast_to(v, (n, *v.shape))
    return lax.all_to_all(stacked, axis, split_axis=0, concat_axis=0, tiled=True)


def dot_nn(a, b):
    return lax.dot_general(a, b, (((1,), (0,)), ((), ())), preferred_element_type=F32)


def dot_nt(a, b):
    return lax.dot_general(a, b, (((1,), (1,)), ((), ())), preferred_element_type=F32)


def exact(dot, a, b):
    high = a.astype(BF)
    low = (a - high.astype(F32)).astype(BF)
    both = dot(jnp.concatenate([high, low], axis=0), b)
    n = a.shape[0]
    return both[:n] + both[n:]


def first_tile(row):
    return row * (row - 1) // 2


SLOTS = 3
TILES = first_tile(HALF)
SPARE = {(1, 0): (1, 7), (2, 0): (2, 6), (2, 1): (2, 7), (3, 0): (0, 6), (3, 1): (3, 7), (3, 2): (0, 7)}


def spot(plane, i, k):
    z = i % 4
    own = i // 4 == plane
    if own or (plane == 0 and k >= z):
        return 8 * z + k
    z, k = SPARE[z, k]
    return 8 * z + k


def plane_pairs():
    pairs = []
    for half in range(2):
        for i in range(HALF):
            for k in range(i):
                plane = i // 4
                source = 64 * half + 32 * plane + spot(plane, i, k)
                target = 64 * half + 32 * (1 - plane) + spot(1 - plane, i, k)
                pairs.append((source, target))
    return pairs


class Leaf:
    def __init__(self, left, right, diag):
        self.left, self.right, self.diag = left, right, diag

    def column(self, j):
        return sum(HALF - 1 - m for m in range(j))

    def u(self, i, k, count=1):
        at = first_tile(i) + k
        return self.left[at : at + count].reshape(-1, self.left.shape[2])

    def vt(self, i, k, count=1):
        at = self.column(k) + i - k - 1
        return self.right[at : at + count].reshape(-1, self.right.shape[2])


class Moves:
    def __init__(self, rows):
        self.rows = rows

    def start(self, i):
        for move in self.rows.get(i, []):
            move.start()

    def wait(self, i):
        for move in self.rows.get(i, []):
            move.wait()


def inverse_moves(leaf, first, inv, sems):
    return Moves(
        {
            n: [pltpu.make_async_copy(inv.at[first + n], leaf.diag.at[n], sems.at[n])]
            for n in range(HALF)
        }
    )


def factor_moves(leaf, kept_left, kept_right, lsems, rsems, keep):
    rows = {}
    for i in range(1, HALF):
        at = first_tile(i)
        pairs = [(kept_left.at[pl.ds(at, i)], leaf.left.at[pl.ds(at, i)], lsems.at[i])]
        for k in range(i):
            place = leaf.column(k) + i - k - 1
            pairs.append((kept_right.at[place], leaf.right.at[place], rsems.at[place]))
        rows[i] = [
            pltpu.make_async_copy(*((b, a) if keep else (a, b)), sem) for a, b, sem in pairs
        ]
    return Moves(rows)


class Loader:
    def __init__(self, leaf, place, tiles, inv, kept, stage, sems, dsems, lsems, rsems):
        self.leaf, self.stage = leaf, stage
        rows = {}
        for i in range(1, HALF):
            rows[i] = []
            for k in range(i):
                one, two = spot(0, i, k), spot(1, i, k)
                rows[i].append(
                    pltpu.make_async_copy(
                        tiles.at[one + place[0] * (two - one)],
                        stage.at[i % SLOTS, k],
                        sems.at[first_tile(i) + k],
                    )
                )
        self.tiles = Moves(rows)
        self.inverse = inverse_moves(leaf, HALF * place[1], inv, dsems)
        self.kept = factor_moves(leaf, *kept, lsems, rsems, True)
        for i in range(SLOTS):
            self.start(i)
        self(0)

    def start(self, i):
        self.inverse.start(i)
        self.tiles.start(i)

    def __call__(self, i):
        leaf = self.leaf
        rank = leaf.left.shape[1]
        self.inverse.wait(i)
        self.tiles.wait(i)
        for k in range(i):
            leaf.left[first_tile(i) + k] = self.stage[i % SLOTS, k, :rank].astype(BF)
            leaf.right[leaf.column(k) + i - k - 1] = self.stage[i % SLOTS, k, rank:].astype(BF)
        self.kept.start(i - 1)
        if i + SLOTS < HALF:
            self.start(i + SLOTS)

    def finish(self):
        self.kept.start(HALF - 1)
        for i in range(HALF):
            self.kept.wait(i)


class Reloader:
    def __init__(self, leaf, place, inv, kept, dsems, lsems, rsems, order):
        self.inverse = inverse_moves(leaf, HALF * place[1], inv, dsems)
        self.factors = factor_moves(leaf, *kept, lsems, rsems, False)
        for i in order:
            self.inverse.start(i)
            self.factors.start(i)
        self(order[0])

    def __call__(self, i):
        self.inverse.wait(i)
        self.factors.wait(i)


def forward(leaf, rhs, load=None):
    solved, narrow = [], []
    partial = rhs[0]
    last = None
    for i in range(HALF):
        acc = partial
        if i:
            acc = acc - dot_nn(last, leaf.u(i, i - 1))
        x = exact(dot_nn, acc, leaf.diag[i])
        if i + 1 < HALF:
            if load:
                load(i + 1)
            partial = rhs[i + 1]
            if i:
                known = [dot_nt(narrow[k], leaf.vt(i + 1, k)).astype(BF) for k in range(i)]
                partial = partial - dot_nn(jnp.concatenate(known, axis=1), leaf.u(i + 1, 0, i))
        solved.append(x)
        narrow.append(x.astype(BF))
        if i + 1 < HALF:
            last = dot_nt(narrow[i], leaf.vt(i + 1, i)).astype(BF)
    return solved


def backward(leaf, rhs, load=None):
    width = leaf.left.shape[1]
    solved = [None] * HALF
    waiting = {j: [] for j in range(HALF)}
    partial = rhs[HALF - 1]
    last = None
    for j in reversed(range(HALF)):
        acc = partial
        if j + 1 < HALF:
            acc = acc - dot_nn(last, leaf.vt(j + 1, j))
        z = exact(dot_nt, acc, leaf.diag[j])
        if j:
            if load:
                load(j - 1)
            partial = rhs[j - 1]
            if waiting[j - 1]:
                known = jnp.concatenate(waiting[j - 1][::-1], axis=1)
                partial = partial - dot_nn(known, leaf.vt(j + 1, j - 1, HALF - 1 - j))
        solved[j] = z
        narrow = z.astype(BF)
        if j:
            last = dot_nt(narrow, leaf.u(j, j - 1)).astype(BF)
        if j > 1:
            others = dot_nt(narrow, leaf.u(j, 0, j - 1)).astype(BF)
            for k in range(j - 1):
                waiting[k].append(others[:, k * width : (k + 1) * width])
    return solved


def put(out, values):
    for i in range(HALF):
        out[i] = values[i]


def load_kernel(place, tiles, inv, rhs, out, kept_left, kept_right, stage, *scratch):
    left, right, diag, sems, dsems, lsems, rsems = scratch
    leaf = Leaf(left, right, diag)
    kept = (kept_left, kept_right)
    load = Loader(leaf, place, tiles, inv, kept, stage, sems, dsems, lsems, rsems)
    put(out, forward(leaf, [rhs[i] for i in range(HALF)], load))
    load.finish()


def both_kernel(place, kept_left, kept_right, inv, rhs, out, left, right, diag, *sems):
    leaf = Leaf(left, right, diag)
    load = Reloader(leaf, place, inv, (kept_left, kept_right), *sems, range(HALF))
    put(out, backward(leaf, forward(leaf, [rhs[i] for i in range(HALF)], load)))


def backward_kernel(place, kept_left, kept_right, inv, rhs, out, left, right, diag, *sems):
    leaf = Leaf(left, right, diag)
    load = Reloader(leaf, place, inv, (kept_left, kept_right), *sems, range(HALF)[::-1])
    put(out, backward(leaf, [rhs[i] for i in range(HALF)], load))


IN_SMEM = pl.BlockSpec(memory_space=pltpu.SMEM)
IN_VMEM = pl.BlockSpec(memory_space=pltpu.VMEM)
IN_HBM = pl.BlockSpec(memory_space=pltpu.HBM)


def limit(mib):
    return pltpu.CompilerParams(vmem_limit_bytes=mib * 1024 * 1024)


def in_hbm(v):
    return pltpu.with_memory_space_constraint(v, pltpu.HBM)


def leaf_scratch(rank, tile):
    return [
        pltpu.VMEM((TILES, rank, tile), BF),
        pltpu.VMEM((TILES, rank, tile), BF),
        pltpu.VMEM((HALF, tile, tile), BF),
    ]


def leaf_sems():
    dma = pltpu.SemaphoreType.DMA
    return [dma((HALF,)), dma((HALF,)), dma((TILES,))]


def load_and_forward(place, tiles, inv, rhs):
    rank, tile = tiles.shape[1] // 2, tiles.shape[2]
    factors = pltpu.HBM((TILES, rank, tile), BF)
    return pl.pallas_call(
        load_kernel,
        out_shape=(jax.ShapeDtypeStruct(rhs.shape, F32), factors, factors),
        in_specs=[IN_SMEM, IN_HBM, IN_HBM, IN_VMEM],
        out_specs=(IN_VMEM, IN_HBM, IN_HBM),
        scratch_shapes=[
            pltpu.VMEM((SLOTS, HALF - 1, 2 * rank, tile), F32),
            *leaf_scratch(rank, tile),
            pltpu.SemaphoreType.DMA((TILES,)),
            *leaf_sems(),
        ],
        compiler_params=limit(36),
    )(place, in_hbm(tiles), in_hbm(inv), rhs)


def solve(body, place, left, right, inv, rhs):
    return pl.pallas_call(
        body,
        out_shape=jax.ShapeDtypeStruct(rhs.shape, F32),
        in_specs=[IN_SMEM, IN_HBM, IN_HBM, IN_HBM, IN_VMEM],
        out_specs=IN_VMEM,
        scratch_shapes=[*leaf_scratch(*left.shape[1:]), *leaf_sems()],
        compiler_params=limit(24),
    )(place, in_hbm(left), in_hbm(right), in_hbm(inv), rhs)


def per_device(
    root_rhs, diag_inv, tile_u, tile_v, tile_rank, child_x, border_t, child_inv, child_blocks
):
    my_row = lax.axis_index(ROW)
    my_col = lax.axis_index(COL)
    ntile = diag_inv.shape[0]
    tile = diag_inv.shape[1]
    rhs_count = root_rhs.shape[0]
    rank_max = tile_u.shape[4]
    n_child = child_x.shape[0]
    nblk = ntile * tile // BLK
    ndev = lax.axis_size(ALL)
    upper = my_row >= HALF
    in_half = my_row % HALF
    half = lax.axis_index("yh")

    left = tile_u[0, 0, 0]
    live = jnp.arange(rank_max)[None, None, :] < tile_rank[0, 0, 0][:, None, None]
    right = jnp.where(live, tile_v[0, 0, 0].astype(F32), 0.0)

    leaf_u = jnp.where(upper, left[1], left[0]).astype(F32)
    leaf_vt = jnp.where(upper, right[1], right[0]).T
    own_tile = with_layout_constraint(jnp.concatenate([leaf_u, leaf_vt], axis=0), ROWS)
    other_tile = lax.ppermute(own_tile, ALL, plane_pairs())
    upward = jnp.einsum("crs,csb->crb", child_x, border_t, preferred_element_type=F32)
    pieces = (
        upward.reshape(n_child, rhs_count, BB, BLK)
        .transpose(1, 0, 2, 3)
        .reshape(rhs_count, n_child * BB, BLK)
    )
    flat_blocks = child_blocks.reshape(-1)
    dense = jnp.zeros((rhs_count, nblk, BLK), F32).at[:, flat_blocks, :].add(pieces)
    width = ntile * tile // ndev
    parts = dense.reshape(rhs_count, 4, ntile * tile // 4).transpose(1, 0, 2)
    mine = lax.all_to_all(parts, ("yh", "yl"), split_axis=0, concat_axis=0, tiled=True)
    mine = mine.sum(axis=0).reshape(rhs_count, 4, tile).transpose(1, 0, 2)
    mine = lax.all_to_all(mine, "z", split_axis=0, concat_axis=0, tiled=True).sum(axis=0)
    mine = mine.reshape(rhs_count, 8, width).transpose(1, 0, 2)
    mine = lax.all_to_all(mine, COL, split_axis=0, concat_axis=0, tiled=True).sum(axis=0)
    share = jnp.where(my_col < in_half, own_tile, other_tile)
    share = with_layout_constraint(share, ROWS)
    tiles = lax.all_gather(share, PLANE)
    place = jnp.stack([lax.axis_index("yl"), half]).astype(jnp.int32)
    child_sum = copies(mine, HALF_ALL).reshape(ndev // 2, rhs_count, width)
    child_sum = child_sum.transpose(1, 0, 2).reshape(rhs_count, HALF, tile).transpose(1, 0, 2)
    given = root_rhs.reshape(rhs_count, ntile, tile)
    given = lax.dynamic_slice_in_dim(given, HALF * half, HALF, 1)
    own_rhs = given.transpose(1, 0, 2).astype(F32) - child_sum

    x_low, kept_left, kept_right = load_and_forward(place, tiles, diag_inv, own_rhs)
    v0 = right[0].astype(BF)
    u0 = left[0]
    x_col = lax.dynamic_index_in_dim(x_low, my_col, 0, keepdims=False)
    x_own = lax.ppermute(x_col, "yh", [(0, 1)])
    x_own = x_own + jnp.where(upper, 0.0, x_col)
    p = dot_nn(x_own.astype(BF), v0).astype(BF)
    row_sum = copies(dot_nn(p, u0), COL).reshape(8, rhs_count, tile).sum(axis=0)
    row_sums = copies(row_sum, HALF_ROW).reshape(HALF, rhs_count, tile)
    z_high = solve(both_kernel, place, kept_left, kept_right, diag_inv, own_rhs - row_sums)

    z_own = lax.dynamic_index_in_dim(z_high, in_half, 0, keepdims=False).astype(BF)
    q = dot_nt(z_own, u0).astype(BF)
    col_sum = copies(dot_nt(q, v0), ROW).reshape(2, HALF, rhs_count, tile)[1].sum(axis=0)
    col_sums = copies(col_sum, COL).reshape(8, rhs_count, tile)
    low_rhs = x_low - col_sums
    z_low = solve(backward_kernel, place, kept_left, kept_right, diag_inv, low_rhs)
    z_mine = jnp.where(upper, z_high, z_low)
    z_other = lax.ppermute(z_mine, "yh", [(0, 1), (1, 0)])
    low_part = jnp.where(upper, z_other, z_mine)
    high_part = jnp.where(upper, z_mine, z_other)
    result = jnp.concatenate([low_part, high_part], axis=0).transpose(1, 0, 2)
    result = result.reshape(rhs_count, ntile * tile)

    start = (my_row * 8 + my_col) * width
    root_part = lax.dynamic_slice_in_dim(result, start, width, 1)
    gathered = result.reshape(rhs_count, nblk, BLK)[:, flat_blocks, :]
    gathered = gathered.reshape(rhs_count, n_child, BB * BLK).astype(BF)
    returned = jnp.einsum("rcb,csb->crs", gathered, border_t, preferred_element_type=F32)
    child_out = child_x.astype(F32) - jnp.einsum(
        "crs,cst->crt", returned, child_inv.astype(F32)
    )
    return (root_part, child_out)


def solution(mesh):
    finer = Mesh(mesh.devices.reshape(2, 2, 4, 4, 2), ALL)
    in_specs = (
        P(),
        P(),
        P(ROW, COL, None, None, None, None),
        P(ROW, COL, None, None, None, None),
        P(ROW, COL, None, None),
        P(ALL, None, None),
        P(ALL, None, None),
        P(ALL, None, None),
        P(ALL, None),
    )
    out_specs = (P(None, ALL), P(ALL, None, None))
    return jax.shard_map(
        per_device, mesh=finer, in_specs=in_specs, out_specs=out_specs, check_vma=False
    )
```

```python
import functools

import jax
import jax.numpy as jnp
from jax import lax
from jax.experimental import pallas as pl
from jax.experimental.layout import Layout, with_layout_constraint
from jax.experimental.pallas import tpu as pltpu
from jax.sharding import Mesh
from jax.sharding import PartitionSpec as P

BLK = 128
BB = 8
ROW = ("yh", "yl", "z")
HALF_ROW = ("yl", "z")
COL = ("x", "c")
PLANE = ("z", "x", "c")
ALL = ("yh", "yl", "z", "x", "c")
HALF_ALL = ("yl", "z", "x", "c")
HALF = 8
BF = jnp.bfloat16
F32 = jnp.float32
ROWS = Layout((0, 1))


def copies(v, axis):
    n = lax.axis_size(axis)
    stacked = jnp.broadcast_to(v, (n, *v.shape))
    return lax.all_to_all(stacked, axis, split_axis=0, concat_axis=0, tiled=True)


def dot_nn(a, b):
    return lax.dot_general(a, b, (((1,), (0,)), ((), ())), preferred_element_type=F32)


def dot_nt(a, b):
    return lax.dot_general(a, b, (((1,), (1,)), ((), ())), preferred_element_type=F32)


def exact(dot, a, b):
    high = a.astype(BF)
    low = (a - high.astype(F32)).astype(BF)
    both = dot(jnp.concatenate([high, low], axis=0), b)
    n = a.shape[0]
    return both[:n] + both[n:]


def first_tile(row):
    return row * (row - 1) // 2


SLOTS = 3
TILES = first_tile(HALF)
SPARE = {(1, 0): (1, 7), (2, 0): (2, 6), (2, 1): (2, 7), (3, 0): (0, 6), (3, 1): (3, 7), (3, 2): (0, 7)}


def spot(plane, i, k):
    z = i % 4
    own = i // 4 == plane
    if own or (plane == 0 and k >= z):
        return 8 * z + k
    z, k = SPARE[z, k]
    return 8 * z + k


def plane_pairs():
    pairs = []
    for half in range(2):
        for i in range(HALF):
            for k in range(i):
                plane = i // 4
                source = 64 * half + 32 * plane + spot(plane, i, k)
                target = 64 * half + 32 * (1 - plane) + spot(1 - plane, i, k)
                pairs.append((source, target))
    return pairs


class Leaf:
    def __init__(self, left, right, diag):
        self.left, self.right, self.diag = left, right, diag

    def column(self, j):
        return sum(HALF - 1 - m for m in range(j))

    def u(self, i, k, count=1):
        at = first_tile(i) + k
        return self.left[at : at + count].reshape(-1, self.left.shape[2])

    def vt(self, i, k, count=1):
        at = self.column(k) + i - k - 1
        return self.right[at : at + count].reshape(-1, self.right.shape[2])


class Moves:
    def __init__(self, rows):
        self.rows = rows

    def start(self, i):
        for move in self.rows.get(i, []):
            move.start()

    def wait(self, i):
        for move in self.rows.get(i, []):
            move.wait()


def inverse_moves(target, first, source, sems):
    return Moves(
        {
            n: [pltpu.make_async_copy(source.at[first + n], target.at[n], sems.at[n])]
            for n in range(HALF)
        }
    )


def factor_moves(leaf, kept_left, kept_right, lsems, rsems, keep):
    rows = {}
    for i in range(1, HALF):
        at = first_tile(i)
        pairs = [(kept_left.at[pl.ds(at, i)], leaf.left.at[pl.ds(at, i)], lsems.at[i])]
        for k in range(i):
            place = leaf.column(k) + i - k - 1
            pairs.append((kept_right.at[place], leaf.right.at[place], rsems.at[place]))
        rows[i] = [
            pltpu.make_async_copy(*((b, a) if keep else (a, b)), sem) for a, b, sem in pairs
        ]
    return Moves(rows)


class Loader:
    def __init__(self, leaf, place, tiles, stage, sems, kept=None, inverse=None):
        self.leaf, self.stage = leaf, stage
        rows = {}
        for i in range(1, HALF):
            rows[i] = []
            for k in range(i):
                one, two = spot(0, i, k), spot(1, i, k)
                rows[i].append(
                    pltpu.make_async_copy(
                        tiles.at[one + place[0] * (two - one)],
                        stage.at[i % SLOTS, k],
                        sems.at[first_tile(i) + k],
                    )
                )
        self.tiles = Moves(rows)
        self.inverse = inverse or Moves({})
        self.kept = kept or Moves({})
        for i in range(SLOTS):
            self.start(i)
        self(0)

    def start(self, i):
        self.inverse.start(i)
        self.tiles.start(i)

    def __call__(self, i):
        leaf = self.leaf
        rank = leaf.left.shape[1]
        self.inverse.wait(i)
        self.tiles.wait(i)
        for k in range(i):
            leaf.left[first_tile(i) + k] = self.stage[i % SLOTS, k, :rank].astype(BF)
            leaf.right[leaf.column(k) + i - k - 1] = self.stage[i % SLOTS, k, rank:].astype(BF)
        self.kept.start(i - 1)
        if i + SLOTS < HALF:
            self.start(i + SLOTS)


class Reloader:
    def __init__(self, inverse, factors, order):
        self.inverse, self.factors = inverse, factors
        for i in order:
            inverse.start(i)
            factors.start(i)
        self(order[0])

    def __call__(self, i):
        self.inverse.wait(i)
        self.factors.wait(i)


def forward(leaf, rhs, load=None):
    solved, narrow = [], []
    partial = rhs[0]
    last = None
    for i in range(HALF):
        acc = partial
        if i:
            acc = acc - dot_nn(last, leaf.u(i, i - 1))
        x = exact(dot_nn, acc, leaf.diag[i])
        if i + 1 < HALF:
            if load:
                load(i + 1)
            partial = rhs[i + 1]
            if i:
                known = [dot_nt(narrow[k], leaf.vt(i + 1, k)).astype(BF) for k in range(i)]
                partial = partial - dot_nn(jnp.concatenate(known, axis=1), leaf.u(i + 1, 0, i))
        solved.append(x)
        narrow.append(x.astype(BF))
        if i + 1 < HALF:
            last = dot_nt(narrow[i], leaf.vt(i + 1, i)).astype(BF)
    return solved


def backward(leaf, rhs, load=None):
    width = leaf.left.shape[1]
    solved = [None] * HALF
    waiting = {j: [] for j in range(HALF)}
    partial = rhs[HALF - 1]
    last = None
    for j in reversed(range(HALF)):
        acc = partial
        if j + 1 < HALF:
            acc = acc - dot_nn(last, leaf.vt(j + 1, j))
        z = exact(dot_nt, acc, leaf.diag[j])
        if j:
            if load:
                load(j - 1)
            partial = rhs[j - 1]
            if waiting[j - 1]:
                known = jnp.concatenate(waiting[j - 1][::-1], axis=1)
                partial = partial - dot_nn(known, leaf.vt(j + 1, j - 1, HALF - 1 - j))
        solved[j] = z
        narrow = z.astype(BF)
        if j:
            last = dot_nt(narrow, leaf.u(j, j - 1)).astype(BF)
        if j > 1:
            others = dot_nt(narrow, leaf.u(j, 0, j - 1)).astype(BF)
            for k in range(j - 1):
                waiting[k].append(others[:, k * width : (k + 1) * width])
    return solved


def put(out, values):
    for i in range(HALF):
        out[i] = values[i]


def values(ref):
    return [ref[i] for i in range(HALF)]


def keep_tiles(leaf, place, tiles, stage, sems, kept, lsems, rsems, out):
    moves = factor_moves(leaf, *kept, lsems, rsems, True)
    load = Loader(leaf, place, tiles, stage, sems, kept=moves)
    total = jnp.zeros(leaf.left.shape[1:], F32)
    for i in range(1, HALF):
        load(i)
        for k in range(i):
            total = total + leaf.u(i, k).astype(F32) + leaf.vt(i, k).astype(F32)
    out[0] = total.reshape(-1, *out.shape[1:]).sum(axis=0)
    moves.start(HALF - 1)
    for i in range(HALF):
        moves.wait(i)


def first_kernel(place, tiles, inv, rhs, out, kept_left, kept_right, stage, *scratch):
    left, right, diag, sems, dsems, lsems, rsems = scratch
    leaf = Leaf(left, right, diag)

    @pl.when(place[1] == 0)
    def _():
        inverse = inverse_moves(diag, 0, inv, dsems)
        load = Loader(leaf, place, tiles, stage, sems, inverse=inverse)
        put(out, forward(leaf, values(rhs), load))

    @pl.when(place[1] == 1)
    def _():
        out[...] = jnp.zeros(out.shape, F32)
        keep_tiles(leaf, place, tiles, stage, sems, (kept_left, kept_right), lsems, rsems, out)


def second_kernel(place, tiles, kept_left, kept_right, inv, rhs, *refs):
    out, next_left, next_right, stage, left, right, diag, sems, dsems, lsems, rsems = refs
    leaf = Leaf(left, right, diag)

    @pl.when(place[1] == 0)
    def _():
        out[...] = jnp.zeros(out.shape, F32)
        keep_tiles(leaf, place, tiles, stage, sems, (next_left, next_right), lsems, rsems, out)

    @pl.when(place[1] == 1)
    def _():
        inverse = inverse_moves(diag, HALF, inv, dsems)
        factors = factor_moves(leaf, kept_left, kept_right, lsems, rsems, False)
        load = Reloader(inverse, factors, range(HALF))
        put(out, backward(leaf, forward(leaf, values(rhs), load)))


def third_kernel(place, kept_left, kept_right, inv, rhs, out, left, right, diag, *sems):
    dsems, lsems, rsems = sems
    leaf = Leaf(left, right, diag)

    @pl.when(place[1] == 0)
    def _():
        inverse = inverse_moves(diag, 0, inv, dsems)
        factors = factor_moves(leaf, kept_left, kept_right, lsems, rsems, False)
        load = Reloader(inverse, factors, range(HALF)[::-1])
        put(out, backward(leaf, values(rhs), load))

    @pl.when(place[1] == 1)
    def _():
        out[...] = jnp.zeros(out.shape, F32)


IN_SMEM = pl.BlockSpec(memory_space=pltpu.SMEM)
IN_VMEM = pl.BlockSpec(memory_space=pltpu.VMEM)
IN_HBM = pl.BlockSpec(memory_space=pltpu.HBM)


def limit(mib):
    return pltpu.CompilerParams(vmem_limit_bytes=mib * 1024 * 1024)


def in_hbm(v):
    return pltpu.with_memory_space_constraint(v, pltpu.HBM)


def solve(body, place, hbm, rhs, keeps, loads):
    tile = rhs.shape[2]
    rank = tile // 4
    dma = pltpu.SemaphoreType.DMA
    solved = jax.ShapeDtypeStruct(rhs.shape, F32)
    factors = pltpu.HBM((TILES, rank, tile), BF)
    return pl.pallas_call(
        body,
        out_shape=(solved, factors, factors) if keeps else solved,
        in_specs=[IN_SMEM, *[IN_HBM] * len(hbm), IN_VMEM],
        out_specs=(IN_VMEM, IN_HBM, IN_HBM) if keeps else IN_VMEM,
        scratch_shapes=[
            *[pltpu.VMEM((SLOTS, HALF - 1, 2 * rank, tile), F32)] * loads,
            *[pltpu.VMEM((TILES, rank, tile), BF)] * 2,
            pltpu.VMEM((HALF, tile, tile), BF),
            *[dma((TILES,))] * loads,
            dma((HALF,)),
            dma((HALF,)),
            dma((TILES,)),
        ],
        compiler_params=limit(28),
    )(place, *[in_hbm(v) for v in hbm], rhs)


def per_device(
    root_rhs, diag_inv, tile_u, tile_v, tile_rank, child_x, border_t, child_inv, child_blocks
):
    my_row = lax.axis_index(ROW)
    my_col = lax.axis_index(COL)
    ntile = diag_inv.shape[0]
    tile = diag_inv.shape[1]
    rhs_count = root_rhs.shape[0]
    rank_max = tile_u.shape[4]
    n_child = child_x.shape[0]
    nblk = ntile * tile // BLK
    ndev = lax.axis_size(ALL)
    upper = my_row >= HALF
    in_half = my_row % HALF
    half = lax.axis_index("yh")

    left = tile_u[0, 0, 0]
    live = jnp.arange(rank_max)[None, None, :] < tile_rank[0, 0, 0][:, None, None]
    right = jnp.where(live, tile_v[0, 0, 0].astype(F32), 0.0)

    leaf_u = jnp.where(upper, left[1], left[0]).astype(F32)
    leaf_vt = jnp.where(upper, right[1], right[0]).T
    own_tile = with_layout_constraint(jnp.concatenate([leaf_u, leaf_vt], axis=0), ROWS)
    other_tile = lax.ppermute(own_tile, ALL, plane_pairs())
    upward = jnp.einsum("crs,csb->crb", child_x, border_t, preferred_element_type=F32)
    pieces = (
        upward.reshape(n_child, rhs_count, BB, BLK)
        .transpose(1, 0, 2, 3)
        .reshape(rhs_count, n_child * BB, BLK)
    )
    flat_blocks = child_blocks.reshape(-1)
    dense = jnp.zeros((rhs_count, nblk, BLK), F32).at[:, flat_blocks, :].add(pieces)
    width = ntile * tile // ndev
    parts = dense.reshape(rhs_count, 4, ntile * tile // 4).transpose(1, 0, 2)
    mine = lax.all_to_all(parts, ("yh", "yl"), split_axis=0, concat_axis=0, tiled=True)
    mine = mine.sum(axis=0).reshape(rhs_count, 4, tile).transpose(1, 0, 2)
    mine = lax.all_to_all(mine, "z", split_axis=0, concat_axis=0, tiled=True).sum(axis=0)
    mine = mine.reshape(rhs_count, 8, width).transpose(1, 0, 2)
    mine = lax.all_to_all(mine, COL, split_axis=0, concat_axis=0, tiled=True).sum(axis=0)
    share = jnp.where(my_col < in_half, own_tile, other_tile)
    share = with_layout_constraint(share, ROWS)
    tiles = lax.all_gather(share, PLANE)
    place = jnp.stack([lax.axis_index("yl"), half]).astype(jnp.int32)
    child_sum = copies(mine, HALF_ALL).reshape(ndev // 2, rhs_count, width)
    child_sum = child_sum.transpose(1, 0, 2).reshape(rhs_count, HALF, tile).transpose(1, 0, 2)
    given = root_rhs.reshape(rhs_count, ntile, tile)
    given = lax.dynamic_slice_in_dim(given, HALF * half, HALF, 1)
    own_rhs = given.transpose(1, 0, 2).astype(F32) - child_sum

    x_low, *kept = solve(first_kernel, place, [tiles, diag_inv], own_rhs, True, 1)
    v0 = right[0].astype(BF)
    u0 = left[0]
    x_col = lax.dynamic_index_in_dim(x_low, my_col, 0, keepdims=False)
    x_own = lax.ppermute(x_col, "yh", [(0, 1)])
    x_own = x_own + jnp.where(upper, 0.0, x_col)
    p = dot_nn(x_own.astype(BF), v0).astype(BF)
    row_sum = copies(dot_nn(p, u0), COL).reshape(8, rhs_count, tile).sum(axis=0)
    row_sums = copies(row_sum, HALF_ROW).reshape(HALF, rhs_count, tile)
    arrays = [tiles, *kept, diag_inv]
    z_high, *kept = solve(second_kernel, place, arrays, own_rhs - row_sums, True, 1)

    z_own = lax.dynamic_index_in_dim(z_high, in_half, 0, keepdims=False).astype(BF)
    q = dot_nt(z_own, u0).astype(BF)
    col_sum = copies(dot_nt(q, v0), ROW).reshape(2, HALF, rhs_count, tile)[1].sum(axis=0)
    col_sums = copies(col_sum, COL).reshape(8, rhs_count, tile)
    low_rhs = x_low - col_sums
    z_low = solve(third_kernel, place, [*kept, diag_inv], low_rhs, False, 0)
    z_mine = jnp.where(upper, z_high, z_low)
    z_other = lax.ppermute(z_mine, "yh", [(0, 1), (1, 0)])
    low_part = jnp.where(upper, z_other, z_mine)
    high_part = jnp.where(upper, z_mine, z_other)
    result = jnp.concatenate([low_part, high_part], axis=0).transpose(1, 0, 2)
    result = result.reshape(rhs_count, ntile * tile)

    start = (my_row * 8 + my_col) * width
    root_part = lax.dynamic_slice_in_dim(result, start, width, 1)
    gathered = result.reshape(rhs_count, nblk, BLK)[:, flat_blocks, :]
    gathered = gathered.reshape(rhs_count, n_child, BB * BLK).astype(BF)
    returned = jnp.einsum("rcb,csb->crs", gathered, border_t, preferred_element_type=F32)
    child_out = child_x.astype(F32) - jnp.einsum(
        "crs,cst->crt", returned, child_inv.astype(F32)
    )
    return (root_part, child_out)


def solution(mesh):
    finer = Mesh(mesh.devices.reshape(2, 2, 4, 4, 2), ALL)
    in_specs = (
        P(),
        P(),
        P(ROW, COL, None, None, None, None),
        P(ROW, COL, None, None, None, None),
        P(ROW, COL, None, None),
        P(ALL, None, None),
        P(ALL, None, None),
        P(ALL, None, None),
        P(ALL, None),
    )
    out_specs = (P(None, ALL), P(ALL, None, None))
    return jax.shard_map(
        per_device, mesh=finer, in_specs=in_specs, out_specs=out_specs, check_vma=False
    )
```
